32 devices in a mesh: rep: 1, ep: 16 (over z, y, x), sub: 2 (over core).
Axes of the slice: x: 2, y: 2, z: 4, core: 2. Of those that a mesh axis runs over, the one named last changes fastest.
Arguments:
- tokens: bfloat16 [256, 5120], P(('rep', 'ep'), 'sub'), may hold values from -6 to 6
- expert_ids: int32 [256, 1], P(('rep', 'ep')), may hold values from 0 to 1; in each aligned block of 16 rows (0 to 15, 16 to 31, ...) at most 16 rows name the same one
- router_score: float32 [256, 1], P(('rep', 'ep')), may hold values from -8 to 8
- expert_gate_up: bfloat16 [5120, 2, 8192], P('sub', None, 'ep'), may hold values from -0.078125 to 0.078125
- expert_down: bfloat16 [8192, 5120], P('ep', 'sub'), may hold values from -0.09375 to 0.09375
- shared_gate_up: bfloat16 [5120, 2, 8192], P('sub', None, 'ep'), may hold values from -0.078125 to 0.078125
- shared_down: bfloat16 [8192, 5120], P('ep', 'sub'), may hold values from -0.0625 to 0.0625
Outputs:
- mixed: bfloat16 [256, 5120], P(('rep', 'ep'), 'sub')
The draws below stay inside these ranges and needn't reach their ends.
Inputs may be any that keep to these rules, and one draw needn't show every extreme that they name: `expert_ids`: in the rows of one index of ep (aligned blocks of 16 rows) no expert is named more than 16 times, a bound that some block reaches.
All inputs are finite; a program needn't handle non-finite values.
Results may differ from the reference program's by a relative error of at most 0.017.
Values may be sent and summed in bfloat16 or wider, within the bound.
A program may use at most 64 MiB of HBM per device.

```python
import math
import jax
import jax.numpy as jnp
import numpy as np
from jax import lax

D = 5120
FF = 4096
FF_SH = 8192
EXP_ROWS = 8
TOK_ROW = 16
EXPERTS = 2
TOKENS = 256
CAP = 16
N_EP = 16


def levels(own_key, extent, shards, smallest, high):
    loudness = 1.0
    for axis_at, blocks in shards:
        heights = jax.random.uniform(jax.random.fold_in(jax.random.fold_in(own_key, 6), axis_at), (blocks,), jnp.float32, smallest / len(shards), high / len(shards))
        loudness = loudness * jnp.repeat(jnp.exp(heights), extent[axis_at] // blocks).reshape((-1,) + (1,) * (len(extent) - 1 - axis_at))
    return loudness


def routed_block(key, own, number, rows, count, top, reach, slope):
    order = jax.random.permutation(key, count)
    packed, common = load_shares(count, rows * top, reach, slope, True), load_shares(count, rows * top, reach, slope, False)
    places = jnp.arange(count)

    def named(lengths, turn):
        used = int((lengths > 0).sum())
        fixed = max(1, used // 4)
        moved = fixed + (places - fixed + turn * (used - fixed)) % max(1, count - fixed)
        return jnp.zeros((count,), jnp.int32).at[order[jnp.where(places < fixed, places, moved)]].set(jnp.asarray(lengths, jnp.int32))

    lengths = jnp.where(number % 4 == 0, named(packed, number // 4), named(common, number - number // 4 - 1))
    mixed = jax.random.permutation(jax.random.fold_in(own, 3), count)
    source_of, sink = mixed[0:count // 2 * 2:2], mixed[1:count // 2 * 2:2]
    room = jnp.minimum(lengths[source_of] - 1, reach - lengths[sink]) // 2
    room = jnp.where((source_of == order[0]) | (sink == order[0]) | (lengths[sink] == 0), 0, jnp.maximum(room, 0))
    moved = jax.random.randint(jax.random.fold_in(own, 4), (count // 2,), 0, 1 << 20) % (room + 1)
    lengths = lengths.at[source_of].add(-moved).at[sink].add(moved)
    labels = jnp.searchsorted(jnp.cumsum(lengths), jnp.arange(rows * top), side="right").astype(jnp.int32)
    listing = labels.reshape(top, rows).T
    listing = listing[jax.random.permutation(jax.random.fold_in(own, 1), rows)]
    turn = jax.random.randint(jax.random.fold_in(own, 2), (rows, 1), 0, top)
    return jnp.take_along_axis(listing, (jnp.arange(top)[None, :] + turn) % top, axis=1)


def load_shares(number_of, total, limit, slope, full):
    weights = [(1 << 20) // math.isqrt(grade ** slope) + 1 for grade in range(1, number_of + 1)]
    largest = limit if full else min(limit, max(-(-total // number_of), total * weights[0] // sum(weights)))
    least = 1 if total - largest >= number_of - 1 else 0
    given, spare = [largest] + [least] * (number_of - 1), total - largest - least * (number_of - 1)
    while spare > 0:
        candidates = [i for i in range(1, number_of) if given[i] < largest] or [i for i in range(1, number_of) if given[i] < limit]
        pool, remaining = sum([weights[i] for i in candidates]), spare
        for i in candidates:
            addition = min(limit - given[i], max(1, remaining * weights[i] // pool), spare)
            given[i] = given[i] + addition
            spare = spare - addition
    return np.array(given)


def centred(own_key, shape, scale, most, shards=(), kind=jnp.bfloat16):
    array = jax.random.normal(own_key, shape, jnp.float32) * scale
    if len(shards) > 0:
        array = levels(own_key, shape, shards, -0.22, 0.18) * array
    return jnp.clip(array, min=-most, max=most).astype(kind)


def setup_inputs(seed: int = 0, part: int = 0) -> dict:
    key_of = jax.random.split(jax.random.key(seed), 8)
    own_keys = jax.random.split(jax.random.fold_in(key_of[7], part), 8)
    tokens = centred(own_keys[0], (TOKENS, D), 1.0, 6.0, ((0, 16), (1, 2)))
    expert_ids_keys = jax.random.split(jax.random.fold_in(own_keys[1], 1), TOKENS // TOK_ROW)
    expert_ids_turns = jax.random.permutation(jax.random.fold_in(own_keys[1], 3), TOKENS // TOK_ROW)
    expert_ids = jax.vmap(lambda own, number: routed_block(jax.random.fold_in(own_keys[1], 2), own, number, TOK_ROW, EXPERTS, 1, CAP, 2))(expert_ids_keys, expert_ids_turns).reshape((TOKENS, 1))
    router_score = centred(own_keys[2], (TOKENS, 1), 2.0, 8.0, ((0, 16),), jnp.float32)
    expert_gate_up = centred(key_of[3], (D, 2, EXPERTS * FF), D ** -0.5, 0.078125, ((0, 2), (2, 16)))
    expert_down = centred(key_of[4], (EXPERTS * FF, D), FF ** -0.5, 0.09375, ((0, 16), (1, 2)))
    shared_gate_up = centred(key_of[5], (D, 2, FF_SH), D ** -0.5, 0.078125, ((0, 2), (2, 16)))
    shared_down = centred(key_of[6], (FF_SH, D), FF_SH ** -0.5, 0.0625, ((0, 16), (1, 2)))
    return {"tokens": tokens, "expert_ids": expert_ids, "router_score": router_score, "expert_gate_up": expert_gate_up, "expert_down": expert_down, "shared_gate_up": shared_gate_up, "shared_down": shared_down}


def slot_ranks(token_ids, experts):
    onehot = (token_ids[..., None] == jnp.arange(experts, dtype=jnp.int32)).astype(jnp.int32)
    before = jnp.cumsum(onehot, axis=-2) - onehot
    return jnp.sum(before * onehot, axis=-1)


def reference(tokens, expert_ids, router_score, expert_gate_up, expert_down, shared_gate_up, shared_down):
    token_ids = expert_ids[:, 0]
    position = slot_ranks(token_ids.reshape(N_EP, TOK_ROW), EXPERTS).reshape(-1)
    row_index = jnp.arange(TOKENS, dtype=jnp.int32) // TOK_ROW
    slot_index = (row_index * CAP + position).astype(jnp.int32)
    total_slots = N_EP * CAP
    gate = jax.nn.sigmoid(router_score)
    weighted = (gate * tokens.astype(jnp.float32)).astype(jnp.bfloat16)
    block_width = FF // EXP_ROWS

    def add_expert(expert, carry):
        chosen = (token_ids == expert)[:, None] & (slot_index[:, None] == jnp.arange(total_slots, dtype=jnp.int32)[None, :])
        select = chosen.astype(jnp.bfloat16)
        slot_rows = lax.dot_general(select, weighted, (((0,), (0,)), ((), ())), preferred_element_type=jnp.float32).astype(jnp.bfloat16)
        start = (expert * FF).astype(jnp.int32)
        gate_cols = lax.dynamic_slice_in_dim(expert_gate_up, start, FF, 2).reshape(D, 2 * FF)
        gate_up = jnp.dot(slot_rows, gate_cols, preferred_element_type=jnp.float32).reshape(total_slots, 2, FF)
        hidden = (jax.nn.silu(gate_up[:, 0]) * gate_up[:, 1]).astype(jnp.bfloat16)
        hidden = hidden.reshape(total_slots, EXP_ROWS, block_width).astype(jnp.float32)
        down_rows = lax.dynamic_slice_in_dim(expert_down, start, FF, 0).reshape(EXP_ROWS, block_width, D).astype(jnp.float32)
        parts = jnp.einsum("skh,khd->ksd", hidden, down_rows).astype(jnp.bfloat16)
        summed = jnp.sum(parts.astype(jnp.float32), axis=0)
        return carry + jnp.dot(select.astype(jnp.float32), summed, precision=lax.Precision.HIGHEST)

    routed = lax.fori_loop(0, EXPERTS, add_expert, jnp.zeros((TOKENS, D), jnp.float32))
    shared_sum = jnp.dot(tokens, shared_gate_up.reshape(D, 2 * FF_SH), preferred_element_type=jnp.float32).reshape(TOKENS, 2, FF_SH)
    shared_hidden = (jax.nn.silu(shared_sum[:, 0]) * shared_sum[:, 1]).astype(jnp.bfloat16)
    shared = jnp.dot(shared_hidden, shared_down, preferred_element_type=jnp.float32)
    return (shared + routed).astype(jnp.bfloat16)
```

```python
import functools
import jax
import jax.numpy as jnp
from jax import lax
from jax.experimental import pallas as pl
from jax.experimental.pallas import tpu as pltpu
from jax.sharding import PartitionSpec as P

EXP_ROWS = 8
GRID_ROWS = 16
META = 128
KCHUNKS = 4


def layer_kernel(
    zn, tokens_ref, ids_ref, score_ref, egu_ref, edn_ref, sgu_ref, sdn_ref, out_ref,
    x_ref, raw_ref, w_ref, dn_ref, gsend_ref, grecv_ref, hid_ref,
    sa1, ra1, sb1, rb1, sa2, ra2, sb2, rb2, acc_ref, zsend, zrecv, id_v, score_v,
    isem, wsem, dsem, ag_send, ag_recv_a, ag_recv_b, g_send, g_recv,
    xy_send, xy_recv, z_send, z_recv,
):
    tr, half = tokens_ref.shape
    hidden = edn_ref.shape[0]
    line = zn * tr
    hw = hidden // 2
    cut = half // 2
    kc = half // KCHUNKS
    rep = lax.axis_index("rep")
    sub = lax.axis_index("sub")
    me = lax.axis_index("ep")
    z = me // 4
    y = (me // 2) % 2
    x = me % 2

    def at(ep, s=None):
        return (rep, ep, sub if s is None else s)

    xn = at(z * 4 + y * 2 + (1 - x))
    yn = at(z * 4 + (1 - y) * 2 + x)
    up = at(jnp.minimum(z + 1, zn - 1) * 4 + y * 2 + x)
    down = at(jnp.maximum(z - 1, 0) * 4 + y * 2 + x)
    partner = at(me, 1 - sub)
    mesh_id = pl.DeviceIdType.MESH

    own = pl.ds(pl.multiple_of(z * tr, tr), tr)
    inputs = [
        pltpu.make_async_copy(tokens_ref, x_ref.at[own, pl.ds(0, half)], isem.at[0]),
        pltpu.make_async_copy(ids_ref, id_v, isem.at[1]),
        pltpu.make_async_copy(score_ref, score_v, isem.at[2]),
    ]
    for c in inputs:
        c.start()

    barrier = pltpu.get_barrier_semaphore()
    for nb in (xn, yn, partner):
        pl.semaphore_signal(barrier, inc=1, device_id=nb, device_id_type=mesh_id)

    @pl.when(z < zn - 1)
    def _():
        pl.semaphore_signal(barrier, inc=1, device_id=up, device_id_type=mesh_id)

    @pl.when(z > 0)
    def _():
        pl.semaphore_signal(barrier, inc=1, device_id=down, device_id_type=mesh_id)

    loads = []
    for m, src in enumerate((egu_ref, sgu_ref)):
        for k in range(KCHUNKS):
            c = pltpu.make_async_copy(
                src.at[pl.ds(k * kc, kc)], raw_ref.at[m, pl.ds(k * kc, kc)], wsem.at[m, k]
            )
            c.start()
            loads.append((m, k, c))
    dloads = []
    for m, src in enumerate((edn_ref, sdn_ref)):
        c = pltpu.make_async_copy(src, dn_ref.at[pl.ds(m * hidden, hidden)], dsem.at[m])
        c.start()
        dloads.append(c)

    eye = lax.broadcasted_iota(jnp.int32, (tr, tr), 0) == lax.broadcasted_iota(
        jnp.int32, (tr, tr), 1
    )
    for c in inputs:
        c.wait()
    gate_row = 1.0 / (1.0 + jnp.exp(-score_v[...]))
    id_row = id_v[...].astype(jnp.float32)
    gate_col = jnp.sum(jnp.where(eye, gate_row, 0.0), axis=1, keepdims=True)
    id_col = jnp.sum(jnp.where(eye, id_row, 0.0), axis=1, keepdims=True)
    gate_hi = gate_col.astype(jnp.bfloat16).astype(jnp.float32)
    lane = lax.broadcasted_iota(jnp.int32, (tr, META), 1)
    meta = jnp.where(
        lane == 0, gate_hi, jnp.where(lane == 1, gate_col - gate_hi, jnp.where(lane == 2, id_col, 0.0))
    )
    x_ref[own, half:] = meta.astype(jnp.bfloat16)

    pl.semaphore_wait(
        barrier, 3 + (z < zn - 1).astype(jnp.int32) + (z > 0).astype(jnp.int32)
    )

    def rows_of(xr, yr, b):
        return pl.ds(pl.multiple_of(((xr * 2 + yr) * zn + b) * tr, tr), tr)

    wide_a, wide_b = pl.ds(0, cut), pl.ds(cut, half + META - cut)

    def copy(src_slot, dst_slot, cols, kind, b, recv, dev):
        return pltpu.make_async_remote_copy(
            src_ref=x_ref.at[rows_of(*src_slot), cols],
            dst_ref=x_ref.at[rows_of(*dst_slot), cols],
            send_sem=ag_send.at[kind, b],
            recv_sem=recv.at[(dst_slot[0] * 2 + dst_slot[1]) * zn + dst_slot[2]],
            device_id=dev, device_id_type=mesh_id,
        )

    def c_up(h, b):
        return copy((0, 0, b), (0, 0, b), (wide_a, wide_b)[h], 8 * h, b, (ag_recv_a, ag_recv_b)[h], up)

    def c_down(h, b):
        return copy((0, 0, b), (0, 0, b), (wide_a, wide_b)[h], 8 * h + 1, b, (ag_recv_a, ag_recv_b)[h], down)

    def c_ay(b):
        return copy((0, 0, b), (0, 1, b), wide_a, 2, b, ag_recv_a, yn)

    def c_ax(yr, b):
        return copy((0, yr, b), (1, yr, b), wide_a, 3 + yr, b, ag_recv_a, xn)

    def c_bx(b):
        return copy((0, 0, b), (1, 0, b), wide_b, 5, b, ag_recv_b, xn)

    def c_by(xr, b):
        return copy((xr, 0, b), (xr, 1, b), wide_b, 6 + xr, b, ag_recv_b, yn)

    def spread(h, b):
        if h == 0:
            c_ay(b).start()
            c_ax(0, b).start()
        else:
            c_bx(b).start()
            c_by(0, b).start()

    def relay(b):
        c_ay(b).wait_recv()
        c_ax(1, b).start()
        c_bx(b).wait_recv()
        c_by(1, b).start()

    pending = list(loads)

    def deinterleave(count):
        for _ in range(min(count, len(pending))):
            m, k, c = pending.pop(0)
            c.wait()
            step = 128 if kc % 128 == 0 else kc

            @pl.loop(0, kc // step)
            def _(i):
                s = pl.ds(pl.multiple_of(k * kc + i * step, step), step)
                pair = raw_ref[m, s].reshape(step, 2 * hidden)
                for j in range(2):
                    for p in range(2):
                        to = (m * 2 + j) * hidden + p * hw
                        w_ref[s, to:to + hw] = pair[:, p * hidden + j * hw:p * hidden + (j + 1) * hw]

    for h in range(2):
        @pl.when(z < zn - 1)
        def _():
            c_up(h, z).start()

        @pl.when(z > 0)
        def _():
            c_down(h, z).start()

    c_ay(z).start()
    c_bx(z).start()
    c_ax(0, z).start()
    c_by(0, z).start()
    deinterleave(4)
    for s in range(1, zn):
        for h in range(2):
            @pl.when(z - s >= 0)
            def _():
                b = jnp.maximum(z - s, 0)
                c_up(h, b).wait_recv()

                @pl.when(z < zn - 1)
                def _():
                    c_up(h, b).start()

                spread(h, b)

            @pl.when(z + s <= zn - 1)
            def _():
                b = jnp.minimum(z + s, zn - 1)
                c_down(h, b).wait_recv()

                @pl.when(z > 0)
                def _():
                    c_down(h, b).start()

                spread(h, b)

        if s == 1:
            relay(z)
        else:
            @pl.when(z - s + 1 >= 0)
            def _():
                relay(jnp.maximum(z - s + 1, 0))

            @pl.when(z + s - 1 <= zn - 1)
            def _():
                relay(jnp.minimum(z + s - 1, zn - 1))

        if s < zn - 1:
            deinterleave(2)

    deinterleave(len(loads))
    groups = ((0, line), (line, 2 * line), (3 * line, line))

    def c_g(r, i):
        part = pl.ds(*groups[r])
        return pltpu.make_async_remote_copy(
            src_ref=gsend_ref.at[i, part], dst_ref=grecv_ref.at[i, part],
            send_sem=g_send.at[r, i], recv_sem=g_recv.at[r, i],
            device_id=partner, device_id_type=mesh_id,
        )

    def gate_up(r):
        part = pl.ds(*groups[r])
        for i in range(4):
            gsend_ref[i, part] = jnp.dot(
                x_ref[part, :half], w_ref[:, i * hidden:(i + 1) * hidden],
                preferred_element_type=jnp.float32,
            ).astype(jnp.bfloat16)
            c_g(r, i).start()

    own_expert = (me // EXP_ROWS).astype(jnp.float32)

    def activate(r):
        part = pl.ds(*groups[r])
        info = x_ref[part, half:].astype(jnp.float32)
        scale = jnp.where(info[:, 2:3] == own_expert, info[:, 0:1] + info[:, 1:2], 0.0)
        for i in range(4):
            c_g(r, i).wait_recv()
            total = gsend_ref[i, part].astype(jnp.float32) + grecv_ref[i, part].astype(jnp.float32)
            if i < 2:
                total = total * scale
            g, u = total[:, :hw], total[:, hw:]
            hid_ref[part, i * hw:(i + 1) * hw] = (g / (1.0 + jnp.exp(-g)) * u).astype(jnp.bfloat16)

    gate_up(0)

    @pl.when(z - zn + 1 >= 0)
    def _():
        relay(jnp.maximum(z - zn + 1, 0))

    @pl.when(z + zn - 1 <= zn - 1)
    def _():
        relay(jnp.minimum(z + zn - 1, zn - 1))

    activate(0)
    for b in range(zn):
        c_ax(0, b).wait_recv()
        c_by(0, b).wait_recv()
    gate_up(1)
    for c in dloads:
        c.wait()

    def product(first, rows, col):
        return jnp.dot(
            hid_ref[pl.ds(first, rows), :], dn_ref[:, col:col + cut],
            preferred_element_type=jnp.float32,
        )

    def block(b):
        return pl.ds(pl.multiple_of(b * tr, tr), tr)

    def c_xy(kind, d):
        src, dst, dev = ((sa1, ra1, xn), (sb1, rb1, yn), (sa2, ra2, yn), (sb2, rb2, xn))[kind % 4]
        rows = pl.ds(pl.multiple_of((line if kind >= 4 else 0) + d * tr, tr), tr)
        return pltpu.make_async_remote_copy(
            src_ref=src.at[rows], dst_ref=dst.at[rows],
            send_sem=xy_send.at[kind, d], recv_sem=xy_recv.at[kind, d],
            device_id=dev, device_id_type=mesh_id,
        )

    order = (3 - 3 * (z // 2), 2 * (1 - z % 2) + z // 2, 1 + z % 2, z)

    activate(1)
    res = product(line, 2 * line, 0)
    sa1[0:line, :] = res[line:].astype(jnp.bfloat16)
    acc_ref[line:2 * line, 0:cut] = res[:line]
    for k in range(zn):
        c_xy(0, order[k]).start()
    res = product(line, 2 * line, cut)
    sb1[0:line, :] = res[:line].astype(jnp.bfloat16)
    acc_ref[2 * line:3 * line, cut:] = res[line:]
    for k in range(zn):
        c_xy(1, order[k]).start()

    for b in range(zn):
        c_ax(1, b).wait_recv()
        c_by(1, b).wait_recv()
    gate_up(2)
    acc_ref[0:line, 0:cut] = product(0, line, 0)
    acc_ref[0:line, cut:] = product(0, line, cut)
    activate(2)
    sa1[line:2 * line, :] = product(3 * line, line, 0).astype(jnp.bfloat16)
    for k in range(zn):
        c_xy(4, order[k]).start()
    sb1[line:2 * line, :] = product(3 * line, line, cut).astype(jnp.bfloat16)
    for k in range(zn):
        c_xy(5, order[k]).start()

    def shifted(base, d):
        return pl.ds(pl.multiple_of(base + d * tr, tr), tr)

    def second(d):
        c_xy(4, d).wait_recv()
        sa2[block(d), :] = (
            acc_ref[shifted(line, d), 0:cut] + ra1[shifted(line, d), :].astype(jnp.float32)
        ).astype(jnp.bfloat16)
        c_xy(2, d).start()
        c_xy(5, d).wait_recv()
        sb2[block(d), :] = (
            acc_ref[shifted(2 * line, d), cut:] + rb1[shifted(line, d), :].astype(jnp.float32)
        ).astype(jnp.bfloat16)
        c_xy(3, d).start()

    def c_z(h, d):
        cols = pl.ds(h * cut, cut)
        return pltpu.make_async_remote_copy(
            src_ref=zsend.at[block(d), cols], dst_ref=zrecv.at[own, cols],
            send_sem=z_send.at[h, d], recv_sem=z_recv.at[h, z],
            device_id=at(d * 4 + y * 2 + x), device_id_type=mesh_id,
        )

    def c_zin(h, b):
        cols = pl.ds(h * cut, cut)
        return pltpu.make_async_remote_copy(
            src_ref=zsend.at[block(b), cols], dst_ref=zrecv.at[block(b), cols],
            send_sem=z_send.at[h, b], recv_sem=z_recv.at[h, b],
            device_id=at(b * 4 + y * 2 + x), device_id_type=mesh_id,
        )

    def settled(h, d):
        cols = slice(h * cut, (h + 1) * cut)
        first, r1, r2 = ((0, ra1, ra2), (1, rb1, rb2))[h]
        c_xy(first, d).wait_recv()
        c_xy(first + 2, d).wait_recv()
        return acc_ref[block(d), cols] + r1[block(d), :].astype(jnp.float32) + r2[
            block(d), :
        ].astype(jnp.float32)

    for k in range(zn):
        second(order[k])
        if k > 0:
            d = order[k - 1]
            for h in range(2):
                zsend[block(d), h * cut:(h + 1) * cut] = settled(h, d).astype(jnp.bfloat16)
                c_z(h, d).start()

    for h in range(2):
        cols = slice(h * cut, (h + 1) * cut)
        total = settled(h, z)
        for b in order[:zn - 1]:
            c_zin(h, b).wait_recv()
            total = total + zrecv[block(b), cols].astype(jnp.float32)
        out_ref[:, cols] = total.astype(out_ref.dtype)

    for b in range(zn):
        for h in range(2):
            @pl.when(jnp.logical_and(z < zn - 1, b <= z))
            def _():
                c_up(h, b).wait_send()

            @pl.when(jnp.logical_and(z > 0, b >= z))
            def _():
                c_down(h, b).wait_send()

        for c in (c_ay(b), c_ax(0, b), c_ax(1, b), c_bx(b), c_by(0, b), c_by(1, b)):
            c.wait_send()
        for h in range(2):
            @pl.when(b != z)
            def _():
                c_z(h, b).wait_send()
        for kind in range(6):
            c_xy(kind, b).wait_send()
    for r in range(3):
        for i in range(4):
            c_g(r, i).wait_send()


def fused_local(
    tokens, expert_ids, router_score, expert_gate_up, expert_down, shared_gate_up, shared_down
):
    tr, half = tokens.shape
    n = lax.axis_size("ep")
    zn = n // 4
    hidden = expert_down.shape[0]
    rows = n * tr
    line = zn * tr
    cut = half // 2
    bf, f32 = jnp.bfloat16, jnp.float32
    vm = pl.BlockSpec(memory_space=pltpu.VMEM)
    hbm = pl.BlockSpec(memory_space=pltpu.HBM)
    dma = pltpu.SemaphoreType.DMA
    return pl.pallas_call(
        functools.partial(layer_kernel, zn),
        out_shape=pltpu.VMEM((tr, half), bf),
        in_specs=[hbm] * 7,
        out_specs=vm,
        scratch_shapes=[
            pltpu.VMEM((rows, half + META), bf),
            pltpu.VMEM((2, half, 2, hidden), bf),
            pltpu.VMEM((half, 4 * hidden), bf),
            pltpu.VMEM((2 * hidden, half), bf),
            pltpu.VMEM((4, rows, hidden), bf),
            pltpu.VMEM((4, rows, hidden), bf),
            pltpu.VMEM((rows, 2 * hidden), bf),
            pltpu.VMEM((2 * line, cut), bf), pltpu.VMEM((2 * line, cut), bf),
            pltpu.VMEM((2 * line, cut), bf), pltpu.VMEM((2 * line, cut), bf),
            pltpu.VMEM((line, cut), bf), pltpu.VMEM((line, cut), bf),
            pltpu.VMEM((line, cut), bf), pltpu.VMEM((line, cut), bf),
            pltpu.VMEM((rows, half), f32),
            pltpu.VMEM((line, half), bf), pltpu.VMEM((line, half), bf),
            pltpu.VMEM((1, tr), jnp.int32), pltpu.VMEM((1, tr), f32), dma((3,)),
            dma((2, KCHUNKS)), dma((2,)), dma((10, zn)), dma((n,)), dma((n,)), dma((3, 4)), dma((3, 4)),
            dma((6, zn)), dma((6, zn)), dma((2, zn)), dma((2, zn)),
        ],
        compiler_params=pltpu.CompilerParams(
            collective_id=0, has_side_effects=True, vmem_limit_bytes=56 * 2**20
        ),
    )(
        tokens, expert_ids.reshape(1, tr), router_score.reshape(1, tr),
        expert_gate_up, expert_down, shared_gate_up, shared_down,
    )


def slot_ranks(token_ids, experts):
    onehot = (token_ids[..., None] == jnp.arange(experts, dtype=jnp.int32)).astype(jnp.int32)
    before = jnp.cumsum(onehot, axis=-2) - onehot
    return jnp.sum(before * onehot, axis=-1)


def local_mlp(slot_rows, expert_gate_up, expert_down):
    hidden_width = expert_down.shape[0]
    gate_cols = expert_gate_up.reshape(expert_gate_up.shape[0], 2 * hidden_width)
    gate_up_sum = jnp.dot(slot_rows, gate_cols, preferred_element_type=jnp.float32)
    gate_up_sum = lax.psum(gate_up_sum.astype(jnp.bfloat16), "sub").astype(jnp.float32)
    gate_up_sum = gate_up_sum.reshape(slot_rows.shape[0], 2, hidden_width)
    hidden = (jax.nn.silu(gate_up_sum[:, 0]) * gate_up_sum[:, 1]).astype(jnp.bfloat16)
    return jnp.dot(hidden, expert_down, preferred_element_type=jnp.float32).astype(jnp.bfloat16)


def local(
    tokens, expert_ids, router_score, expert_gate_up, expert_down, shared_gate_up, shared_down
):
    rows_here, half_width = tokens.shape
    rows_ep = lax.axis_size("ep")
    experts = rows_ep // EXP_ROWS
    capacity = min(rows_here, max(2, 3 * rows_here // experts))
    shared_width = shared_down.shape[0]
    shared_in = shared_gate_up.reshape(half_width, 2 * shared_width)
    routed_extra = None
    all_tokens, all_ids, all_scores = (
        lax.all_gather(tokens, "ep", axis=0, tiled=True),
        lax.all_gather(expert_ids, "ep", axis=0, tiled=True),
        lax.all_gather(router_score.astype(jnp.bfloat16), "ep", axis=0, tiled=True).astype(
            router_score.dtype
        ),
    )
    shared_sum = jnp.dot(all_tokens, shared_in, preferred_element_type=jnp.float32)
    token_ids = all_ids[:, 0].reshape(rows_ep, rows_here)
    position = slot_ranks(token_ids, experts)
    own_expert = lax.axis_index("ep") // EXP_ROWS
    row_index = lax.broadcasted_iota(jnp.int32, (rows_ep, rows_here), 0)
    slot_index = jnp.where(token_ids == own_expert, row_index * capacity + position, -1).reshape(-1)
    slot_iota = lax.broadcasted_iota(jnp.int32, (rows_ep * capacity, rows_ep * rows_here), 0)
    select = (slot_iota == slot_index[None, :]).astype(jnp.bfloat16)
    weighted = (jax.nn.sigmoid(all_scores) * all_tokens.astype(jnp.float32)).astype(jnp.bfloat16)
    slot_rows = jnp.dot(select, weighted, preferred_element_type=jnp.float32).astype(jnp.bfloat16)
    results = local_mlp(slot_rows, expert_gate_up, expert_down)
    routed_extra = lax.dot_general(
        select, results, (((0,), (0,)), ((), ())), preferred_element_type=jnp.float32
    )
    shared_sum = lax.psum(shared_sum.astype(jnp.bfloat16), "sub").astype(jnp.float32)
    shared_sum = shared_sum.reshape(-1, 2, shared_width)
    shared_hidden = (jax.nn.silu(shared_sum[:, 0]) * shared_sum[:, 1]).astype(jnp.bfloat16)
    partial_value = jnp.dot(shared_hidden, shared_down, preferred_element_type=jnp.float32)
    partial_value = partial_value + routed_extra
    mixed = lax.psum_scatter(partial_value, "ep", scatter_dimension=0, tiled=True)
    return mixed.astype(jnp.bfloat16)


def solution(mesh):
    placed = (
        P(("rep", "ep"), "sub"),
        P(("rep", "ep"), None),
        P(("rep", "ep"), None),
        P("sub", None, "ep"),
        P("ep", "sub"),
        P("sub", None, "ep"),
        P("ep", "sub"),
    )
    fused = mesh.shape["ep"] == GRID_ROWS
    return jax.shard_map(
        fused_local if fused else local, mesh=mesh, in_specs=placed, out_specs=P(("rep", "ep"), "sub"), check_vma=False
    )
```

```python
import functools
import jax
import jax.numpy as jnp
from jax import lax
from jax.experimental import pallas as pl
from jax.experimental.pallas import tpu as pltpu
from jax.sharding import PartitionSpec as P

EXP_ROWS = 8
GRID_ROWS = 16
META = 128
KCHUNKS = 4


def layer_kernel(
    zn, tokens_ref, ids_ref, score_ref, egu_ref, edn_ref, sgu_ref, sdn_ref, out_ref,
    x_ref, raw_ref, w_ref, dn_ref, gsend_ref, grecv_ref, hid_ref,
    sa1, ra1, sb1, rb1, sa2, ra2, sb2, rb2, acc_ref, zsend, zrecv, id_v, score_v,
    isem, wsem, dsem, ag_send, ag_recv, far_recv, send, g_recv, early_recv, xy_recv, z_recv,
):
    tr, half = tokens_ref.shape
    hidden = edn_ref.shape[0]
    line = zn * tr
    hw = hidden // 2
    cut = half // 2
    kc = half // KCHUNKS
    rep = lax.axis_index("rep")
    sub = lax.axis_index("sub")
    me = lax.axis_index("ep")
    z = me // 4
    y = (me // 2) % 2
    x = me % 2

    def at(ep, s=None):
        return (rep, ep, sub if s is None else s)

    xn = at(z * 4 + y * 2 + (1 - x))
    yn = at(z * 4 + (1 - y) * 2 + x)
    up = at(jnp.minimum(z + 1, zn - 1) * 4 + y * 2 + x)
    down = at(jnp.maximum(z - 1, 0) * 4 + y * 2 + x)
    partner = at(me, 1 - sub)
    mesh_id = pl.DeviceIdType.MESH

    own = pl.ds(pl.multiple_of(z * tr, tr), tr)
    inputs = [
        pltpu.make_async_copy(tokens_ref, x_ref.at[own, pl.ds(0, half)], isem.at[0]),
        pltpu.make_async_copy(ids_ref, id_v, isem.at[1]),
        pltpu.make_async_copy(score_ref, score_v, isem.at[2]),
    ]
    for c in inputs:
        c.start()

    barrier = pltpu.get_barrier_semaphore()
    for nb in (xn, yn, partner):
        pl.semaphore_signal(barrier, inc=1, device_id=nb, device_id_type=mesh_id)

    @pl.when(z < zn - 1)
    def _():
        pl.semaphore_signal(barrier, inc=1, device_id=up, device_id_type=mesh_id)

    @pl.when(z > 0)
    def _():
        pl.semaphore_signal(barrier, inc=1, device_id=down, device_id_type=mesh_id)

    loads = []
    for m, src in enumerate((egu_ref, sgu_ref)):
        for k in range(KCHUNKS):
            c = pltpu.make_async_copy(
                src.at[pl.ds(k * kc, kc)], raw_ref.at[m, pl.ds(k * kc, kc)], wsem.at[m, k]
            )
            c.start()
            loads.append((m, k, c))
    dloads = []
    for m, src in enumerate((edn_ref, sdn_ref)):
        c = pltpu.make_async_copy(src, dn_ref.at[pl.ds(m * hidden, hidden)], dsem.at[m])
        c.start()
        dloads.append(c)

    eye = lax.broadcasted_iota(jnp.int32, (tr, tr), 0) == lax.broadcasted_iota(
        jnp.int32, (tr, tr), 1
    )
    for c in inputs:
        c.wait()
    gate_row = 1.0 / (1.0 + jnp.exp(-score_v[...]))
    id_row = id_v[...].astype(jnp.float32)
    gate_col = jnp.sum(jnp.where(eye, gate_row, 0.0), axis=1, keepdims=True)
    id_col = jnp.sum(jnp.where(eye, id_row, 0.0), axis=1, keepdims=True)
    gate_hi = gate_col.astype(jnp.bfloat16).astype(jnp.float32)
    lane = lax.broadcasted_iota(jnp.int32, (tr, META), 1)
    meta = jnp.where(
        lane == 0, gate_hi, jnp.where(lane == 1, gate_col - gate_hi, jnp.where(lane == 2, id_col, 0.0))
    )
    x_ref[own, half:] = meta.astype(jnp.bfloat16)

    pl.semaphore_wait(
        barrier, 3 + (z < zn - 1).astype(jnp.int32) + (z > 0).astype(jnp.int32)
    )

    def rows_of(xr, yr, b):
        return pl.ds(pl.multiple_of(((xr * 2 + yr) * zn + b) * tr, tr), tr)

    wide_a, wide_b = pl.ds(0, cut), pl.ds(cut, half + META - cut)

    def copy(src_slot, dst_slot, cols, kind, recv, dev):
        return pltpu.make_async_remote_copy(
            src_ref=x_ref.at[rows_of(*src_slot), cols],
            dst_ref=x_ref.at[rows_of(*dst_slot), cols],
            send_sem=ag_send.at[kind], recv_sem=recv,
            device_id=dev, device_id_type=mesh_id,
        )

    def c_up(h, b):
        return copy((0, 0, b), (0, 0, b), (wide_a, wide_b)[h], 1, ag_recv.at[h, b], up)

    def c_down(h, b):
        return copy((0, 0, b), (0, 0, b), (wide_a, wide_b)[h], 2, ag_recv.at[h, b], down)

    def c_ay(b):
        return copy((0, 0, b), (0, 1, b), wide_a, 0, ag_recv.at[2, b], yn)

    def c_ax(yr, b):
        return copy((0, yr, b), (1, yr, b), wide_a, 0, far_recv.at[0, yr], xn)

    def c_bx(b):
        return copy((0, 0, b), (1, 0, b), wide_b, 0, ag_recv.at[3, b], xn)

    def c_by(xr, b):
        return copy((xr, 0, b), (xr, 1, b), wide_b, 0, far_recv.at[1, xr], yn)

    def far_wait(kind, r):
        rows = pl.ds((3 if r else (2, 1)[kind]) * line, line)
        part = x_ref.at[rows, (wide_a, wide_b)[kind]]
        pltpu.make_async_copy(part, part, far_recv.at[kind, r]).wait()

    def spread(h, b):
        if h == 0:
            c_ay(b).start()
            c_ax(0, b).start()
        else:
            c_bx(b).start()
            c_by(0, b).start()

    def relay(b):
        c_ay(b).wait_recv()
        c_ax(1, b).start()
        c_bx(b).wait_recv()
        c_by(1, b).start()

    pending = list(loads)

    def deinterleave(count):
        for _ in range(min(count, len(pending))):
            m, k, c = pending.pop(0)
            c.wait()
            step = 128 if kc % 128 == 0 else kc

            @pl.loop(0, kc // step)
            def _(i):
                s = pl.ds(pl.multiple_of(k * kc + i * step, step), step)
                w_ref[s, m * 2 * hidden:(m + 1) * 2 * hidden] = raw_ref[m, s].reshape(
                    step, 2 * hidden
                )

    for h in range(2):
        @pl.when(z < zn - 1)
        def _():
            c_up(h, z).start()

        @pl.when(z > 0)
        def _():
            c_down(h, z).start()

    c_ay(z).start()
    c_bx(z).start()
    c_ax(0, z).start()
    c_by(0, z).start()
    deinterleave(4)
    for s in range(1, zn):
        for h in range(2):
            @pl.when(z - s >= 0)
            def _():
                b = jnp.maximum(z - s, 0)
                c_up(h, b).wait_recv()

                @pl.when(z < zn - 1)
                def _():
                    c_up(h, b).start()

                spread(h, b)

            @pl.when(z + s <= zn - 1)
            def _():
                b = jnp.minimum(z + s, zn - 1)
                c_down(h, b).wait_recv()

                @pl.when(z > 0)
                def _():
                    c_down(h, b).start()

                spread(h, b)

        if s == 1:
            relay(z)
        else:
            @pl.when(z - s + 1 >= 0)
            def _():
                relay(jnp.maximum(z - s + 1, 0))

            @pl.when(z + s - 1 <= zn - 1)
            def _():
                relay(jnp.minimum(z + s - 1, zn - 1))

        if s < zn - 1:
            deinterleave(2)

    deinterleave(len(loads))
    groups = ((0, line), (line, 2 * line), (3 * line, line))

    def c_g(r, i):
        part = pl.ds(*groups[r])
        return pltpu.make_async_remote_copy(
            src_ref=gsend_ref.at[i, part], dst_ref=grecv_ref.at[i, part],
            send_sem=send.at[0], recv_sem=g_recv.at[r, i],
            device_id=partner, device_id_type=mesh_id,
        )

    def gate_up(r):
        part = pl.ds(*groups[r])
        for i in range(2):
            gsend_ref[i, part] = jnp.dot(
                x_ref[part, :half], w_ref[:, i * 2 * hidden:(i + 1) * 2 * hidden],
                preferred_element_type=jnp.float32,
            ).astype(jnp.bfloat16)
            c_g(r, i).start()

    own_expert = (me // EXP_ROWS).astype(jnp.float32)

    def activate(r):
        part = pl.ds(*groups[r])
        info = x_ref[part, half:].astype(jnp.float32)
        scale = jnp.where(info[:, 2:3] == own_expert, info[:, 0:1] + info[:, 1:2], 0.0)
        for i in range(2):
            c_g(r, i).wait_recv()
            for j in range(2):
                g, u = (
                    gsend_ref[i, part, c:c + hw].astype(jnp.float32)
                    + grecv_ref[i, part, c:c + hw].astype(jnp.float32)
                    for c in (j * hw, hidden + j * hw)
                )
                if i == 0:
                    g, u = g * scale, u * scale
                col = i * hidden + j * hw
                hid_ref[part, col:col + hw] = (g / (1.0 + jnp.exp(-g)) * u).astype(jnp.bfloat16)

    gate_up(0)

    @pl.when(z - zn + 1 >= 0)
    def _():
        relay(jnp.maximum(z - zn + 1, 0))

    @pl.when(z + zn - 1 <= zn - 1)
    def _():
        relay(jnp.minimum(z + zn - 1, zn - 1))

    activate(0)
    far_wait(0, 0)
    far_wait(1, 0)
    gate_up(1)
    for c in dloads:
        c.wait()

    def product(first, rows, col=0, width=half):
        return jnp.dot(
            hid_ref[pl.ds(first, rows), :], dn_ref[:, col:col + width],
            preferred_element_type=jnp.float32,
        )

    def block(b):
        return pl.ds(pl.multiple_of(b * tr, tr), tr)

    def c_xy(kind, d):
        src, dst, dev = ((sa1, ra1, xn), (sb1, rb1, yn), (sa2, ra2, yn), (sb2, rb2, xn))[kind % 4]
        rows = pl.ds(pl.multiple_of((line if kind >= 4 else 0) + d * tr, tr), tr)
        return pltpu.make_async_remote_copy(
            src_ref=src.at[rows], dst_ref=dst.at[rows],
            send_sem=send.at[1],
            recv_sem=early_recv.at[kind] if kind < 2 else xy_recv.at[kind - 2, d],
            device_id=dev, device_id_type=mesh_id,
        )

    order = (3 - 3 * (z // 2), 2 * (1 - z % 2) + z // 2, 1 + z % 2, z)

    acc_ref[0:line, 0:cut] = product(0, line, 0, cut)
    activate(1)
    res = product(line, 2 * line)
    sa1[0:line, :] = res[line:, :cut].astype(jnp.bfloat16)
    sb1[0:line, :] = res[:line, cut:].astype(jnp.bfloat16)
    for k in range(zn):
        c_xy(0, order[k]).start()
        c_xy(1, order[k]).start()
    acc_ref[line:2 * line, 0:cut] = res[:line, :cut]
    acc_ref[2 * line:3 * line, cut:] = res[line:, cut:]
    far_wait(0, 1)
    far_wait(1, 1)
    gate_up(2)
    acc_ref[0:line, cut:] = product(0, line, cut, cut)
    activate(2)
    res = product(3 * line, line).astype(jnp.bfloat16)
    sa1[line:2 * line, :] = res[:, :cut]
    sb1[line:2 * line, :] = res[:, cut:]
    for k in range(zn):
        c_xy(4, order[k]).start()
        c_xy(5, order[k]).start()

    def shifted(base, d):
        return pl.ds(pl.multiple_of(base + d * tr, tr), tr)

    def second(d):
        c_xy(4, d).wait_recv()
        sa2[block(d), :] = (
            acc_ref[shifted(line, d), 0:cut] + ra1[shifted(line, d), :].astype(jnp.float32)
        ).astype(jnp.bfloat16)
        c_xy(2, d).start()
        c_xy(5, d).wait_recv()
        sb2[block(d), :] = (
            acc_ref[shifted(2 * line, d), cut:] + rb1[shifted(line, d), :].astype(jnp.float32)
        ).astype(jnp.bfloat16)
        c_xy(3, d).start()

    def c_z(h, d):
        cols = pl.ds(h * cut, cut)
        return pltpu.make_async_remote_copy(
            src_ref=zsend.at[block(d), cols], dst_ref=zrecv.at[own, cols],
            send_sem=send.at[2], recv_sem=z_recv.at[h],
            device_id=at(d * 4 + y * 2 + x), device_id_type=mesh_id,
        )

    def arrived(sem, part):
        pltpu.make_async_copy(part, part, sem).wait()

    def settled(h, d):
        cols = slice(h * cut, (h + 1) * cut)
        first, r1, r2 = ((0, ra1, ra2), (1, rb1, rb2))[h]
        c_xy(first + 2, d).wait_recv()
        return acc_ref[block(d), cols] + r1[block(d), :].astype(jnp.float32) + r2[
            block(d), :
        ].astype(jnp.float32)

    for k in range(zn):
        second(order[k])
    arrived(early_recv.at[0], ra1.at[pl.ds(0, line)])
    arrived(early_recv.at[1], rb1.at[pl.ds(0, line)])
    for k in range(zn - 1):
        d = order[k]
        for h in range(2):
            zsend[block(d), h * cut:(h + 1) * cut] = settled(h, d).astype(jnp.bfloat16)
            c_z(h, d).start()

    for h in range(2):
        cols = slice(h * cut, (h + 1) * cut)
        total = settled(h, z)
        arrived(z_recv.at[h], zrecv.at[pl.ds(0, line - tr), pl.ds(h * cut, cut)])
        for b in order[:zn - 1]:
            total = total + zrecv[block(b), cols].astype(jnp.float32)
        out_ref[:, cols] = total.astype(out_ref.dtype)

    def sent(sem, part):
        pltpu.make_async_remote_copy(
            src_ref=part, dst_ref=part, send_sem=sem, recv_sem=z_recv.at[0],
            device_id=partner, device_id_type=mesh_id,
        ).wait_send()

    for b in range(zn):
        @pl.when(jnp.logical_and(z < zn - 1, b == z))
        def _():
            sent(ag_send.at[1], x_ref.at[pl.ds(0, (b + 1) * tr)])

        @pl.when(jnp.logical_and(z > 0, b == z))
        def _():
            sent(ag_send.at[2], x_ref.at[pl.ds(0, (zn - b) * tr)])

    sent(ag_send.at[0], x_ref.at[pl.ds(0, 3 * line)])
    sent(send.at[0], gsend_ref)
    sent(send.at[1], x_ref.at[pl.ds(0, 3 * line), pl.ds(0, half)])
    sent(send.at[2], zsend.at[pl.ds(0, line - tr)])


def fused_local(
    tokens, expert_ids, router_score, expert_gate_up, expert_down, shared_gate_up, shared_down
):
    tr, half = tokens.shape
    n = lax.axis_size("ep")
    zn = n // 4
    hidden = expert_down.shape[0]
    rows = n * tr
    line = zn * tr
    cut = half // 2
    bf, f32 = jnp.bfloat16, jnp.float32
    vm = pl.BlockSpec(memory_space=pltpu.VMEM)
    hbm = pl.BlockSpec(memory_space=pltpu.HBM)
    dma = pltpu.SemaphoreType.DMA
    return pl.pallas_call(
        functools.partial(layer_kernel, zn),
        out_shape=pltpu.VMEM((tr, half), bf),
        in_specs=[hbm] * 7,
        out_specs=vm,
        scratch_shapes=[
            pltpu.VMEM((rows, half + META), bf),
            pltpu.VMEM((2, half, 2, hidden), bf),
            pltpu.VMEM((half, 4 * hidden), bf),
            pltpu.VMEM((2 * hidden, half), bf),
            pltpu.VMEM((2, rows, 2 * hidden), bf),
            pltpu.VMEM((2, rows, 2 * hidden), bf),
            pltpu.VMEM((rows, 2 * hidden), bf),
            pltpu.VMEM((2 * line, cut), bf), pltpu.VMEM((2 * line, cut), bf),
            pltpu.VMEM((2 * line, cut), bf), pltpu.VMEM((2 * line, cut), bf),
            pltpu.VMEM((line, cut), bf), pltpu.VMEM((line, cut), bf),
            pltpu.VMEM((line, cut), bf), pltpu.VMEM((line, cut), bf),
            pltpu.VMEM((rows, half), f32),
            pltpu.VMEM((line, half), bf), pltpu.VMEM((line, half), bf),
            pltpu.VMEM((1, tr), jnp.int32), pltpu.VMEM((1, tr), f32), dma((3,)),
            dma((2, KCHUNKS)), dma((2,)), dma((3,)), dma((4, zn)), dma((2, 2)), dma((3,)), dma((3, 2)),
            dma((2,)), dma((4, zn)), dma((2,)),
        ],
        compiler_params=pltpu.CompilerParams(
            collective_id=0, has_side_effects=True, vmem_limit_bytes=56 * 2**20
        ),
    )(
        tokens, expert_ids.reshape(1, tr), router_score.reshape(1, tr),
        expert_gate_up, expert_down, shared_gate_up, shared_down,
    )


def slot_ranks(token_ids, experts):
    onehot = (token_ids[..., None] == jnp.arange(experts, dtype=jnp.int32)).astype(jnp.int32)
    before = jnp.cumsum(onehot, axis=-2) - onehot
    return jnp.sum(before * onehot, axis=-1)


def local_mlp(slot_rows, expert_gate_up, expert_down):
    hidden_width = expert_down.shape[0]
    gate_cols = expert_gate_up.reshape(expert_gate_up.shape[0], 2 * hidden_width)
    gate_up_sum = jnp.dot(slot_rows, gate_cols, preferred_element_type=jnp.float32)
    gate_up_sum = lax.psum(gate_up_sum.astype(jnp.bfloat16), "sub").astype(jnp.float32)
    gate_up_sum = gate_up_sum.reshape(slot_rows.shape[0], 2, hidden_width)
    hidden = (jax.nn.silu(gate_up_sum[:, 0]) * gate_up_sum[:, 1]).astype(jnp.bfloat16)
    return jnp.dot(hidden, expert_down, preferred_element_type=jnp.float32).astype(jnp.bfloat16)


def local(
    tokens, expert_ids, router_score, expert_gate_up, expert_down, shared_gate_up, shared_down
):
    rows_here, half_width = tokens.shape
    rows_ep = lax.axis_size("ep")
    experts = rows_ep // EXP_ROWS
    capacity = min(rows_here, max(2, 3 * rows_here // experts))
    shared_width = shared_down.shape[0]
    shared_in = shared_gate_up.reshape(half_width, 2 * shared_width)
    routed_extra = None
    all_tokens, all_ids, all_scores = (
        lax.all_gather(tokens, "ep", axis=0, tiled=True),
        lax.all_gather(expert_ids, "ep", axis=0, tiled=True),
        lax.all_gather(router_score.astype(jnp.bfloat16), "ep", axis=0, tiled=True).astype(
            router_score.dtype
        ),
    )
    shared_sum = jnp.dot(all_tokens, shared_in, preferred_element_type=jnp.float32)
    token_ids = all_ids[:, 0].reshape(rows_ep, rows_here)
    position = slot_ranks(token_ids, experts)
    own_expert = lax.axis_index("ep") // EXP_ROWS
    row_index = lax.broadcasted_iota(jnp.int32, (rows_ep, rows_here), 0)
    slot_index = jnp.where(token_ids == own_expert, row_index * capacity + position, -1).reshape(-1)
    slot_iota = lax.broadcasted_iota(jnp.int32, (rows_ep * capacity, rows_ep * rows_here), 0)
    select = (slot_iota == slot_index[None, :]).astype(jnp.bfloat16)
    weighted = (jax.nn.sigmoid(all_scores) * all_tokens.astype(jnp.float32)).astype(jnp.bfloat16)
    slot_rows = jnp.dot(select, weighted, preferred_element_type=jnp.float32).astype(jnp.bfloat16)
    results = local_mlp(slot_rows, expert_gate_up, expert_down)
    routed_extra = lax.dot_general(
        select, results, (((0,), (0,)), ((), ())), preferred_element_type=jnp.float32
    )
    shared_sum = lax.psum(shared_sum.astype(jnp.bfloat16), "sub").astype(jnp.float32)
    shared_sum = shared_sum.reshape(-1, 2, shared_width)
    shared_hidden = (jax.nn.silu(shared_sum[:, 0]) * shared_sum[:, 1]).astype(jnp.bfloat16)
    partial_value = jnp.dot(shared_hidden, shared_down, preferred_element_type=jnp.float32)
    partial_value = partial_value + routed_extra
    mixed = lax.psum_scatter(partial_value, "ep", scatter_dimension=0, tiled=True)
    return mixed.astype(jnp.bfloat16)


def solution(mesh):
    placed = (
        P(("rep", "ep"), "sub"),
        P(("rep", "ep"), None),
        P(("rep", "ep"), None),
        P("sub", None, "ep"),
        P("ep", "sub"),
        P("sub", None, "ep"),
        P("ep", "sub"),
    )
    fused = mesh.shape["ep"] == GRID_ROWS
    return jax.shard_map(
        fused_local if fused else local, mesh=mesh, in_specs=placed, out_specs=P(("rep", "ep"), "sub"), check_vma=False
    )
```

```python
import functools
import jax
import jax.numpy as jnp
from jax import lax
from jax.experimental import pallas as pl
from jax.experimental.pallas import tpu as pltpu
from jax.sharding import PartitionSpec as P

EXP_ROWS = 8
GRID_ROWS = 16
META = 128
KCHUNKS = 4


def layer_kernel(
    zn, tokens_ref, ids_ref, score_ref, egu_ref, edn_ref, sgu_ref, sdn_ref, out_ref,
    x_ref, raw_ref, w_ref, dn_ref, gsend_ref, grecv_ref, hid_ref,
    sa1, ra1, sb1, rb1, sa2, ra2, sb2, rb2, acc_ref, zsend, zrecv, cs, cr, ps, pr, id_v, score_v,
    isem, wsem, dsem, ag_send, ag_recv, far_recv, send, g_recv, early_recv, xy_recv, z_recv, c_recv, p_recv,
):
    tr, half = tokens_ref.shape
    hidden = edn_ref.shape[0]
    line = zn * tr
    hw = hidden // 2
    cut = half // 2
    third = sa1.shape[1]
    both = 2 * third
    kc = half // KCHUNKS
    rep = lax.axis_index("rep")
    sub = lax.axis_index("sub")
    me = lax.axis_index("ep")
    z = me // 4
    y = (me // 2) % 2
    x = me % 2

    def at(ep, s=None):
        return (rep, ep, sub if s is None else s)

    xn = at(z * 4 + y * 2 + (1 - x))
    yn = at(z * 4 + (1 - y) * 2 + x)
    up = at(jnp.minimum(z + 1, zn - 1) * 4 + y * 2 + x)
    down = at(jnp.maximum(z - 1, 0) * 4 + y * 2 + x)
    diag = at(z * 4 + (1 - y) * 2 + (1 - x))
    partner = at(me, 1 - sub)
    mesh_id = pl.DeviceIdType.MESH

    own = pl.ds(pl.multiple_of(z * tr, tr), tr)
    inputs = [
        pltpu.make_async_copy(tokens_ref, x_ref.at[own, pl.ds(0, half)], isem.at[0]),
        pltpu.make_async_copy(ids_ref, id_v, isem.at[1]),
        pltpu.make_async_copy(score_ref, score_v, isem.at[2]),
    ]
    for c in inputs:
        c.start()

    barrier = pltpu.get_barrier_semaphore()
    for nb in (xn, yn, partner):
        pl.semaphore_signal(barrier, inc=1, device_id=nb, device_id_type=mesh_id)

    @pl.when(z < zn - 1)
    def _():
        pl.semaphore_signal(barrier, inc=1, device_id=up, device_id_type=mesh_id)

    @pl.when(z > 0)
    def _():
        pl.semaphore_signal(barrier, inc=1, device_id=down, device_id_type=mesh_id)

    loads = []
    for m, src in enumerate((egu_ref, sgu_ref)):
        for k in range(KCHUNKS):
            c = pltpu.make_async_copy(
                src.at[pl.ds(k * kc, kc)], raw_ref.at[m, pl.ds(k * kc, kc)], wsem.at[m, k]
            )
            c.start()
            loads.append((m, k, c))
    dloads = []
    for m, src in enumerate((edn_ref, sdn_ref)):
        c = pltpu.make_async_copy(src, dn_ref.at[pl.ds(m * hidden, hidden)], dsem.at[m])
        c.start()
        dloads.append(c)

    eye = lax.broadcasted_iota(jnp.int32, (tr, tr), 0) == lax.broadcasted_iota(
        jnp.int32, (tr, tr), 1
    )
    for c in inputs:
        c.wait()
    gate_row = 1.0 / (1.0 + jnp.exp(-score_v[...]))
    id_row = id_v[...].astype(jnp.float32)
    gate_col = jnp.sum(jnp.where(eye, gate_row, 0.0), axis=1, keepdims=True)
    id_col = jnp.sum(jnp.where(eye, id_row, 0.0), axis=1, keepdims=True)
    gate_hi = gate_col.astype(jnp.bfloat16).astype(jnp.float32)
    lane = lax.broadcasted_iota(jnp.int32, (tr, META), 1)
    meta = jnp.where(
        lane == 0, gate_hi, jnp.where(lane == 1, gate_col - gate_hi, jnp.where(lane == 2, id_col, 0.0))
    )
    x_ref[own, half:] = meta.astype(jnp.bfloat16)

    pl.semaphore_wait(
        barrier, 3 + (z < zn - 1).astype(jnp.int32) + (z > 0).astype(jnp.int32)
    )

    def rows_of(xr, yr, b):
        return pl.ds(pl.multiple_of(((xr * 2 + yr) * zn + b) * tr, tr), tr)

    wide_a, wide_b = pl.ds(0, cut), pl.ds(cut, half + META - cut)

    def copy(src_slot, dst_slot, cols, kind, recv, dev):
        return pltpu.make_async_remote_copy(
            src_ref=x_ref.at[rows_of(*src_slot), cols],
            dst_ref=x_ref.at[rows_of(*dst_slot), cols],
            send_sem=ag_send.at[kind], recv_sem=recv,
            device_id=dev, device_id_type=mesh_id,
        )

    def c_up(h, b):
        return copy((0, 0, b), (0, 0, b), (wide_a, wide_b)[h], 1, ag_recv.at[h, b], up)

    def c_down(h, b):
        return copy((0, 0, b), (0, 0, b), (wide_a, wide_b)[h], 2, ag_recv.at[h, b], down)

    def c_ay(b):
        return copy((0, 0, b), (0, 1, b), wide_a, 0, ag_recv.at[2, b], yn)

    def c_ax(yr, b):
        return copy((0, yr, b), (1, yr, b), wide_a, 0, far_recv.at[0, yr], xn)

    def c_bx(b):
        return copy((0, 0, b), (1, 0, b), wide_b, 0, ag_recv.at[3, b], xn)

    def c_by(xr, b):
        return copy((xr, 0, b), (xr, 1, b), wide_b, 0, far_recv.at[1, xr], yn)

    def far_wait(kind, r):
        rows = pl.ds((3 if r else (2, 1)[kind]) * line, line)
        part = x_ref.at[rows, (wide_a, wide_b)[kind]]
        pltpu.make_async_copy(part, part, far_recv.at[kind, r]).wait()

    def spread(h, b):
        if h == 0:
            c_ay(b).start()
            c_ax(0, b).start()
        else:
            c_bx(b).start()
            c_by(0, b).start()

    def relay(b):
        c_ay(b).wait_recv()
        c_ax(1, b).start()
        c_bx(b).wait_recv()
        c_by(1, b).start()

    pending = list(loads)

    def deinterleave(count):
        for _ in range(min(count, len(pending))):
            m, k, c = pending.pop(0)
            c.wait()
            step = 128 if kc % 128 == 0 else kc

            @pl.loop(0, kc // step)
            def _(i):
                s = pl.ds(pl.multiple_of(k * kc + i * step, step), step)
                w_ref[s, m * 2 * hidden:(m + 1) * 2 * hidden] = raw_ref[m, s].reshape(
                    step, 2 * hidden
                )

    for h in range(2):
        @pl.when(z < zn - 1)
        def _():
            c_up(h, z).start()

        @pl.when(z > 0)
        def _():
            c_down(h, z).start()

    c_ay(z).start()
    c_bx(z).start()
    c_ax(0, z).start()
    c_by(0, z).start()
    deinterleave(4)
    for s in range(1, zn):
        for h in range(2):
            @pl.when(z - s >= 0)
            def _():
                b = jnp.maximum(z - s, 0)
                c_up(h, b).wait_recv()

                @pl.when(z < zn - 1)
                def _():
                    c_up(h, b).start()

                spread(h, b)

            @pl.when(z + s <= zn - 1)
            def _():
                b = jnp.minimum(z + s, zn - 1)
                c_down(h, b).wait_recv()

                @pl.when(z > 0)
                def _():
                    c_down(h, b).start()

                spread(h, b)

        if s == 1:
            relay(z)
        else:
            @pl.when(z - s + 1 >= 0)
            def _():
                relay(jnp.maximum(z - s + 1, 0))

            @pl.when(z + s - 1 <= zn - 1)
            def _():
                relay(jnp.minimum(z + s - 1, zn - 1))

        if s < zn - 1:
            deinterleave(2)

    deinterleave(len(loads))
    groups = ((0, line), (line, 2 * line), (3 * line, line))

    def c_g(r, i):
        part = pl.ds(*groups[r])
        return pltpu.make_async_remote_copy(
            src_ref=gsend_ref.at[i, part], dst_ref=grecv_ref.at[i, part],
            send_sem=send.at[0], recv_sem=g_recv.at[r, i],
            device_id=partner, device_id_type=mesh_id,
        )

    def gate_up(r):
        part = pl.ds(*groups[r])
        for i in range(2):
            gsend_ref[i, part] = jnp.dot(
                x_ref[part, :half], w_ref[:, i * 2 * hidden:(i + 1) * 2 * hidden],
                preferred_element_type=jnp.float32,
            ).astype(jnp.bfloat16)
            c_g(r, i).start()

    own_expert = (me // EXP_ROWS).astype(jnp.float32)

    def activate(r):
        part = pl.ds(*groups[r])
        info = x_ref[part, half:].astype(jnp.float32)
        scale = jnp.where(info[:, 2:3] == own_expert, info[:, 0:1] + info[:, 1:2], 0.0)
        for i in range(2):
            c_g(r, i).wait_recv()
            for j in range(2):
                g, u = (
                    gsend_ref[i, part, c:c + hw].astype(jnp.float32)
                    + grecv_ref[i, part, c:c + hw].astype(jnp.float32)
                    for c in (j * hw, hidden + j * hw)
                )
                if i == 0:
                    g, u = g * scale, u * scale
                col = i * hidden + j * hw
                hid_ref[part, col:col + hw] = (g / (1.0 + jnp.exp(-g)) * u).astype(jnp.bfloat16)

    gate_up(0)

    @pl.when(z - zn + 1 >= 0)
    def _():
        relay(jnp.maximum(z - zn + 1, 0))

    @pl.when(z + zn - 1 <= zn - 1)
    def _():
        relay(jnp.minimum(z + zn - 1, zn - 1))

    activate(0)
    far_wait(0, 0)
    far_wait(1, 0)
    gate_up(1)
    for c in dloads:
        c.wait()

    def product(first, rows, col=0, width=half):
        return jnp.dot(
            hid_ref[pl.ds(first, rows), :], dn_ref[:, col:col + width],
            preferred_element_type=jnp.float32,
        )

    def block(b):
        return pl.ds(pl.multiple_of(b * tr, tr), tr)

    def c_xy(kind, d):
        src, dst, dev = ((sa1, ra1, xn), (sb1, rb1, yn), (sa2, ra2, yn), (sb2, rb2, xn))[kind % 4]
        rows = pl.ds(pl.multiple_of((line if kind >= 4 else 0) + d * tr, tr), tr)
        return pltpu.make_async_remote_copy(
            src_ref=src.at[rows], dst_ref=dst.at[rows],
            send_sem=send.at[1],
            recv_sem=early_recv.at[kind] if kind < 2 else xy_recv.at[kind - 2, d],
            device_id=dev, device_id_type=mesh_id,
        )

    order = (3 - 3 * (z // 2), 2 * (1 - z % 2) + z // 2, 1 + z % 2, z)

    def arrived(sem, part):
        pltpu.make_async_copy(part, part, sem).wait()

    def c_c(first, count, d):
        return pltpu.make_async_remote_copy(
            src_ref=cs.at[pl.ds(first, count), d], dst_ref=cr.at[z, pl.ds(first, count)],
            send_sem=send.at[3], recv_sem=c_recv.at[first],
            device_id=at(d * 4 + y * 2 + x), device_id_type=mesh_id,
        )

    def along(first, count, res):
        rows = slice(first * line, (first + count) * line)
        acc_ref[rows, both:] = res
        cs[first:first + count] = res.astype(jnp.bfloat16).reshape(count, zn, tr, half - both)
        for d in order[:zn - 1]:
            c_c(first, count, d).start()

    res = product(0, line, third, half - third)
    along(0, 1, res[:, third:])
    acc_ref[0:line, third:both] = res[:, :third]
    activate(1)
    res = product(line, 2 * line)
    sa1[0:line, :] = res[line:, :third].astype(jnp.bfloat16)
    sb1[0:line, :] = res[:line, third:both].astype(jnp.bfloat16)
    for k in range(zn):
        c_xy(0, order[k]).start()
        c_xy(1, order[k]).start()
    along(1, 2, res[:, both:])
    acc_ref[line:2 * line, 0:third] = res[:line, :third]
    acc_ref[2 * line:3 * line, third:both] = res[line:, third:both]
    far_wait(0, 1)
    far_wait(1, 1)
    gate_up(2)
    acc_ref[0:line, 0:third] = product(0, line, 0, third)
    activate(2)
    res = product(3 * line, line)
    sa1[line:2 * line, :] = res[:, :third].astype(jnp.bfloat16)
    sb1[line:2 * line, :] = res[:, third:both].astype(jnp.bfloat16)
    for k in range(zn):
        c_xy(4, order[k]).start()
        c_xy(5, order[k]).start()
    along(3, 1, res[:, both:])

    def shifted(base, d):
        return pl.ds(pl.multiple_of(base + d * tr, tr), tr)

    def second(d):
        c_xy(4, d).wait_recv()
        sa2[block(d), :] = (
            acc_ref[shifted(line, d), 0:third] + ra1[shifted(line, d), :].astype(jnp.float32)
        ).astype(jnp.bfloat16)
        c_xy(2, d).start()
        c_xy(5, d).wait_recv()
        sb2[block(d), :] = (
            acc_ref[shifted(2 * line, d), third:both] + rb1[shifted(line, d), :].astype(jnp.float32)
        ).astype(jnp.bfloat16)
        c_xy(3, d).start()

    def c_z(h, d):
        cols = pl.ds(h * third, third)
        return pltpu.make_async_remote_copy(
            src_ref=zsend.at[block(d), cols], dst_ref=zrecv.at[own, cols],
            send_sem=send.at[2], recv_sem=z_recv.at[h],
            device_id=at(d * 4 + y * 2 + x), device_id_type=mesh_id,
        )

    def summed(c):
        total = acc_ref[shifted(c * line, z), both:]
        for b in order[:zn - 1]:
            total = total + cr[b, c].astype(jnp.float32)
        return total

    def c_p(c):
        return pltpu.make_async_remote_copy(
            src_ref=ps.at[c - 1], dst_ref=pr.at[c - 1],
            send_sem=send.at[4], recv_sem=p_recv.at[0],
            device_id=(yn, xn, diag)[c - 1], device_id_type=mesh_id,
        )

    def settled(h, d):
        cols = slice(h * third, (h + 1) * third)
        first, r1, r2 = ((0, ra1, ra2), (1, rb1, rb2))[h]
        c_xy(first + 2, d).wait_recv()
        return acc_ref[block(d), cols] + r1[block(d), :].astype(jnp.float32) + r2[
            block(d), :
        ].astype(jnp.float32)

    for k in range(zn):
        second(order[k])
    for first, count in ((0, 1), (1, 2), (3, 1)):
        arrived(c_recv.at[first], cr.at[pl.ds(0, zn - 1), pl.ds(0, count)])
    for c in (1, 2, 3):
        ps[c - 1] = summed(c).astype(jnp.bfloat16)
        c_p(c).start()
    arrived(early_recv.at[0], ra1.at[pl.ds(0, line)])
    arrived(early_recv.at[1], rb1.at[pl.ds(0, line)])
    for k in range(zn - 1):
        d = order[k]
        for h in range(2):
            zsend[block(d), h * third:(h + 1) * third] = settled(h, d).astype(jnp.bfloat16)
            c_z(h, d).start()

    total = summed(0)
    arrived(p_recv.at[0], pr)
    for c in range(3):
        total = total + pr[c].astype(jnp.float32)
    out_ref[:, both:] = total.astype(out_ref.dtype)
    for h in range(2):
        cols = slice(h * third, (h + 1) * third)
        total = settled(h, z)
        arrived(z_recv.at[h], zrecv.at[pl.ds(0, line - tr), pl.ds(h * third, third)])
        for b in order[:zn - 1]:
            total = total + zrecv[block(b), cols].astype(jnp.float32)
        out_ref[:, cols] = total.astype(out_ref.dtype)

    def sent(sem, part):
        pltpu.make_async_remote_copy(
            src_ref=part, dst_ref=part, send_sem=sem, recv_sem=z_recv.at[0],
            device_id=partner, device_id_type=mesh_id,
        ).wait_send()

    for b in range(zn):
        @pl.when(jnp.logical_and(z < zn - 1, b == z))
        def _():
            sent(ag_send.at[1], x_ref.at[pl.ds(0, (b + 1) * tr)])

        @pl.when(jnp.logical_and(z > 0, b == z))
        def _():
            sent(ag_send.at[2], x_ref.at[pl.ds(0, (zn - b) * tr)])

    sent(ag_send.at[0], x_ref.at[pl.ds(0, 3 * line)])
    sent(send.at[0], gsend_ref)
    sent(send.at[1], x_ref.at[pl.ds(0, 3 * line), pl.ds(0, both)])
    sent(send.at[3], cs.at[pl.ds(0, zn - 1)])
    sent(send.at[4], ps)
    sent(send.at[2], zsend.at[pl.ds(0, line - tr)])


def fused_local(
    tokens, expert_ids, router_score, expert_gate_up, expert_down, shared_gate_up, shared_down
):
    tr, half = tokens.shape
    n = lax.axis_size("ep")
    zn = n // 4
    hidden = expert_down.shape[0]
    rows = n * tr
    line = zn * tr
    third = half * 7 // 20 // 128 * 128
    bf, f32 = jnp.bfloat16, jnp.float32
    vm = pl.BlockSpec(memory_space=pltpu.VMEM)
    hbm = pl.BlockSpec(memory_space=pltpu.HBM)
    dma = pltpu.SemaphoreType.DMA
    return pl.pallas_call(
        functools.partial(layer_kernel, zn),
        out_shape=pltpu.VMEM((tr, half), bf),
        in_specs=[hbm] * 7,
        out_specs=vm,
        scratch_shapes=[
            pltpu.VMEM((rows, half + META), bf),
            pltpu.VMEM((2, half, 2, hidden), bf),
            pltpu.VMEM((half, 4 * hidden), bf),
            pltpu.VMEM((2 * hidden, half), bf),
            pltpu.VMEM((2, rows, 2 * hidden), bf),
            pltpu.VMEM((2, rows, 2 * hidden), bf),
            pltpu.VMEM((rows, 2 * hidden), bf),
            pltpu.VMEM((2 * line, third), bf), pltpu.VMEM((2 * line, third), bf),
            pltpu.VMEM((2 * line, third), bf), pltpu.VMEM((2 * line, third), bf),
            pltpu.VMEM((line, third), bf), pltpu.VMEM((line, third), bf),
            pltpu.VMEM((line, third), bf), pltpu.VMEM((line, third), bf),
            pltpu.VMEM((rows, half), f32),
            pltpu.VMEM((line, 2 * third), bf), pltpu.VMEM((line, 2 * third), bf),
            pltpu.VMEM((4, zn, tr, half - 2 * third), bf), pltpu.VMEM((zn, 4, tr, half - 2 * third), bf),
            pltpu.VMEM((3, tr, half - 2 * third), bf), pltpu.VMEM((3, tr, half - 2 * third), bf),
            pltpu.VMEM((1, tr), jnp.int32), pltpu.VMEM((1, tr), f32), dma((3,)),
            dma((2, KCHUNKS)), dma((2,)), dma((3,)), dma((4, zn)), dma((2, 2)), dma((5,)), dma((3, 2)),
            dma((2,)), dma((4, zn)), dma((2,)), dma((4,)), dma((1,)),
        ],
        compiler_params=pltpu.CompilerParams(
            collective_id=0, has_side_effects=True, vmem_limit_bytes=56 * 2**20
        ),
    )(
        tokens, expert_ids.reshape(1, tr), router_score.reshape(1, tr),
        expert_gate_up, expert_down, shared_gate_up, shared_down,
    )


def slot_ranks(token_ids, experts):
    onehot = (token_ids[..., None] == jnp.arange(experts, dtype=jnp.int32)).astype(jnp.int32)
    before = jnp.cumsum(onehot, axis=-2) - onehot
    return jnp.sum(before * onehot, axis=-1)


def local_mlp(slot_rows, expert_gate_up, expert_down):
    hidden_width = expert_down.shape[0]
    gate_cols = expert_gate_up.reshape(expert_gate_up.shape[0], 2 * hidden_width)
    gate_up_sum = jnp.dot(slot_rows, gate_cols, preferred_element_type=jnp.float32)
    gate_up_sum = lax.psum(gate_up_sum.astype(jnp.bfloat16), "sub").astype(jnp.float32)
    gate_up_sum = gate_up_sum.reshape(slot_rows.shape[0], 2, hidden_width)
    hidden = (jax.nn.silu(gate_up_sum[:, 0]) * gate_up_sum[:, 1]).astype(jnp.bfloat16)
    return jnp.dot(hidden, expert_down, preferred_element_type=jnp.float32).astype(jnp.bfloat16)


def local(
    tokens, expert_ids, router_score, expert_gate_up, expert_down, shared_gate_up, shared_down
):
    rows_here, half_width = tokens.shape
    rows_ep = lax.axis_size("ep")
    experts = rows_ep // EXP_ROWS
    capacity = min(rows_here, max(2, 3 * rows_here // experts))
    shared_width = shared_down.shape[0]
    shared_in = shared_gate_up.reshape(half_width, 2 * shared_width)
    routed_extra = None
    all_tokens, all_ids, all_scores = (
        lax.all_gather(tokens, "ep", axis=0, tiled=True),
        lax.all_gather(expert_ids, "ep", axis=0, tiled=True),
        lax.all_gather(router_score.astype(jnp.bfloat16), "ep", axis=0, tiled=True).astype(
            router_score.dtype
        ),
    )
    shared_sum = jnp.dot(all_tokens, shared_in, preferred_element_type=jnp.float32)
    token_ids = all_ids[:, 0].reshape(rows_ep, rows_here)
    position = slot_ranks(token_ids, experts)
    own_expert = lax.axis_index("ep") // EXP_ROWS
    row_index = lax.broadcasted_iota(jnp.int32, (rows_ep, rows_here), 0)
    slot_index = jnp.where(token_ids == own_expert, row_index * capacity + position, -1).reshape(-1)
    slot_iota = lax.broadcasted_iota(jnp.int32, (rows_ep * capacity, rows_ep * rows_here), 0)
    select = (slot_iota == slot_index[None, :]).astype(jnp.bfloat16)
    weighted = (jax.nn.sigmoid(all_scores) * all_tokens.astype(jnp.float32)).astype(jnp.bfloat16)
    slot_rows = jnp.dot(select, weighted, preferred_element_type=jnp.float32).astype(jnp.bfloat16)
    results = local_mlp(slot_rows, expert_gate_up, expert_down)
    routed_extra = lax.dot_general(
        select, results, (((0,), (0,)), ((), ())), preferred_element_type=jnp.float32
    )
    shared_sum = lax.psum(shared_sum.astype(jnp.bfloat16), "sub").astype(jnp.float32)
    shared_sum = shared_sum.reshape(-1, 2, shared_width)
    shared_hidden = (jax.nn.silu(shared_sum[:, 0]) * shared_sum[:, 1]).astype(jnp.bfloat16)
    partial_value = jnp.dot(shared_hidden, shared_down, preferred_element_type=jnp.float32)
    partial_value = partial_value + routed_extra
    mixed = lax.psum_scatter(partial_value, "ep", scatter_dimension=0, tiled=True)
    return mixed.astype(jnp.bfloat16)


def solution(mesh):
    placed = (
        P(("rep", "ep"), "sub"),
        P(("rep", "ep"), None),
        P(("rep", "ep"), None),
        P("sub", None, "ep"),
        P("ep", "sub"),
        P("sub", None, "ep"),
        P("ep", "sub"),
    )
    fused = mesh.shape["ep"] == GRID_ROWS
    return jax.shard_map(
        fused_local if fused else local, mesh=mesh, in_specs=placed, out_specs=P(("rep", "ep"), "sub"), check_vma=False
    )
```

```python
import functools
import jax
import jax.numpy as jnp
from jax import lax
from jax.experimental import pallas as pl
from jax.experimental.pallas import tpu as pltpu
from jax.sharding import PartitionSpec as P

EXP_ROWS = 8
GRID_ROWS = 16
META = 128
KCHUNKS = 4


def layer_kernel(
    zn, tokens_ref, ids_ref, score_ref, egu_ref, edn_ref, sgu_ref, sdn_ref, out_ref,
    x_ref, raw_ref, w_ref, dn_ref, gsend_ref, grecv_ref, hid_ref,
    sa1, ra1, sb1, rb1, sa2, ra2, sb2, rb2, acc_ref, zsend, zrecv, cs, cr, ps, pr, id_v, score_v,
    isem, wsem, dsem, ag_send, ag_recv, far_recv, send, g_recv, early_recv, xy_recv, z_recv, c_recv, p_recv,
):
    tr, half = tokens_ref.shape
    hidden = edn_ref.shape[0]
    line = zn * tr
    hw = hidden // 2
    cut = half // 2
    third = sa1.shape[1]
    both = 2 * third
    kc = half // KCHUNKS
    rep = lax.axis_index("rep")
    sub = lax.axis_index("sub")
    me = lax.axis_index("ep")
    z = me // 4
    y = (me // 2) % 2
    x = me % 2

    def at(ep, s=None):
        return (rep, ep, sub if s is None else s)

    xn = at(z * 4 + y * 2 + (1 - x))
    yn = at(z * 4 + (1 - y) * 2 + x)
    up = at(jnp.minimum(z + 1, zn - 1) * 4 + y * 2 + x)
    down = at(jnp.maximum(z - 1, 0) * 4 + y * 2 + x)
    diag = at(z * 4 + (1 - y) * 2 + (1 - x))
    partner = at(me, 1 - sub)
    mesh_id = pl.DeviceIdType.MESH

    own = pl.ds(pl.multiple_of(z * tr, tr), tr)
    inputs = [
        pltpu.make_async_copy(tokens_ref, x_ref.at[own, pl.ds(0, half)], isem.at[0]),
        pltpu.make_async_copy(ids_ref, id_v, isem.at[1]),
        pltpu.make_async_copy(score_ref, score_v, isem.at[2]),
    ]
    for c in inputs:
        c.start()

    barrier = pltpu.get_barrier_semaphore()
    for nb in (xn, yn, partner):
        pl.semaphore_signal(barrier, inc=1, device_id=nb, device_id_type=mesh_id)

    @pl.when(z < zn - 1)
    def _():
        pl.semaphore_signal(barrier, inc=1, device_id=up, device_id_type=mesh_id)

    @pl.when(z > 0)
    def _():
        pl.semaphore_signal(barrier, inc=1, device_id=down, device_id_type=mesh_id)

    loads = []
    for m, src in enumerate((egu_ref, sgu_ref)):
        for k in range(KCHUNKS):
            c = pltpu.make_async_copy(
                src.at[pl.ds(k * kc, kc)], raw_ref.at[m, pl.ds(k * kc, kc)], wsem.at[m, k]
            )
            c.start()
            loads.append((m, k, c))
    dloads = []
    for m, src in enumerate((edn_ref, sdn_ref)):
        c = pltpu.make_async_copy(src, dn_ref.at[pl.ds(m * hidden, hidden)], dsem.at[m])
        c.start()
        dloads.append(c)

    eye = lax.broadcasted_iota(jnp.int32, (tr, tr), 0) == lax.broadcasted_iota(
        jnp.int32, (tr, tr), 1
    )
    for c in inputs:
        c.wait()
    gate_row = 1.0 / (1.0 + jnp.exp(-score_v[...]))
    id_row = id_v[...].astype(jnp.float32)
    gate_col = jnp.sum(jnp.where(eye, gate_row, 0.0), axis=1, keepdims=True)
    id_col = jnp.sum(jnp.where(eye, id_row, 0.0), axis=1, keepdims=True)
    gate_hi = gate_col.astype(jnp.bfloat16).astype(jnp.float32)
    lane = lax.broadcasted_iota(jnp.int32, (tr, META), 1)
    meta = jnp.where(
        lane == 0, gate_hi, jnp.where(lane == 1, gate_col - gate_hi, jnp.where(lane == 2, id_col, 0.0))
    )
    x_ref[own, half:] = meta.astype(jnp.bfloat16)

    pl.semaphore_wait(
        barrier, 3 + (z < zn - 1).astype(jnp.int32) + (z > 0).astype(jnp.int32)
    )

    def rows_of(xr, yr, b):
        return pl.ds(pl.multiple_of(((xr * 2 + yr) * zn + b) * tr, tr), tr)

    wide_a, wide_b = pl.ds(0, cut), pl.ds(cut, half + META - cut)
    piece_w = cut // 2 // 128 * 128
    parts = (
        pl.ds(0, piece_w), pl.ds(piece_w, cut - piece_w),
        pl.ds(cut, piece_w), pl.ds(cut + piece_w, half + META - cut - piece_w),
    )

    def copy(src_slot, dst_slot, cols, kind, recv, dev):
        return pltpu.make_async_remote_copy(
            src_ref=x_ref.at[rows_of(*src_slot), cols],
            dst_ref=x_ref.at[rows_of(*dst_slot), cols],
            send_sem=ag_send.at[kind], recv_sem=recv,
            device_id=dev, device_id_type=mesh_id,
        )

    def c_up(h, b):
        return copy((0, 0, b), (0, 0, b), parts[h], 1, ag_recv.at[h, b], up)

    def c_down(h, b):
        return copy((0, 0, b), (0, 0, b), parts[h], 2, ag_recv.at[h, b], down)

    def c_ay(b):
        return copy((0, 0, b), (0, 1, b), wide_a, 0, ag_recv.at[4, b], yn)

    def c_ax(yr, b):
        return copy((0, yr, b), (1, yr, b), wide_a, 0, far_recv.at[0, yr], xn)

    def c_bx(b):
        return copy((0, 0, b), (1, 0, b), wide_b, 0, ag_recv.at[5, b], xn)

    def c_by(xr, b):
        return copy((xr, 0, b), (xr, 1, b), wide_b, 0, far_recv.at[1, xr], yn)

    def far_wait(kind, r):
        rows = pl.ds((3 if r else (2, 1)[kind]) * line, line)
        part = x_ref.at[rows, (wide_a, wide_b)[kind]]
        pltpu.make_async_copy(part, part, far_recv.at[kind, r]).wait()

    def spread(h, b):
        if h == 0:
            c_ay(b).start()
            c_ax(0, b).start()
        else:
            c_bx(b).start()
            c_by(0, b).start()

    def relay(b):
        c_ay(b).wait_recv()
        c_ax(1, b).start()
        c_bx(b).wait_recv()
        c_by(1, b).start()

    pending = list(loads)

    def deinterleave(count):
        for _ in range(min(count, len(pending))):
            m, k, c = pending.pop(0)
            c.wait()
            step = 128 if kc % 128 == 0 else kc

            @pl.loop(0, kc // step)
            def _(i):
                s = pl.ds(pl.multiple_of(k * kc + i * step, step), step)
                w_ref[s, m * 2 * hidden:(m + 1) * 2 * hidden] = raw_ref[m, s].reshape(
                    step, 2 * hidden
                )

    for h in range(4):
        @pl.when(z < zn - 1)
        def _():
            c_up(h, z).start()

        @pl.when(z > 0)
        def _():
            c_down(h, z).start()

    c_ay(z).start()
    c_bx(z).start()
    c_ax(0, z).start()
    c_by(0, z).start()
    deinterleave(4)
    for s in range(1, zn):
        for h in range(4):
            @pl.when(z - s >= 0)
            def _():
                b = jnp.maximum(z - s, 0)
                c_up(h, b).wait_recv()

                @pl.when(z < zn - 1)
                def _():
                    c_up(h, b).start()

                if h % 2:
                    spread(h // 2, b)

            @pl.when(z + s <= zn - 1)
            def _():
                b = jnp.minimum(z + s, zn - 1)
                c_down(h, b).wait_recv()

                @pl.when(z > 0)
                def _():
                    c_down(h, b).start()

                if h % 2:
                    spread(h // 2, b)

        if s == 1:
            relay(z)
        else:
            @pl.when(z - s + 1 >= 0)
            def _():
                relay(jnp.maximum(z - s + 1, 0))

            @pl.when(z + s - 1 <= zn - 1)
            def _():
                relay(jnp.minimum(z + s - 1, zn - 1))

        if s < zn - 1:
            deinterleave(2)

    deinterleave(len(loads))
    groups = ((0, line), (line, 2 * line), (3 * line, line))

    def c_g(r, i):
        part = pl.ds(*groups[r])
        return pltpu.make_async_remote_copy(
            src_ref=gsend_ref.at[i, part], dst_ref=grecv_ref.at[i, part],
            send_sem=send.at[0], recv_sem=g_recv.at[r, i],
            device_id=partner, device_id_type=mesh_id,
        )

    def gate_up(r):
        part = pl.ds(*groups[r])
        for i in range(2):
            lead = line if r == 2 else 0
            rows = pl.ds(groups[r][0] - lead, groups[r][1] + lead)
            gsend_ref[i, part] = jnp.dot(
                x_ref[rows, :half], w_ref[:, i * 2 * hidden:(i + 1) * 2 * hidden],
                preferred_element_type=jnp.float32,
            )[lead:].astype(jnp.bfloat16)
            c_g(r, i).start()

    own_expert = (me // EXP_ROWS).astype(jnp.float32)

    def activate(r, i):
        part = pl.ds(*groups[r])
        if i == 0:
            info = x_ref[part, half:].astype(jnp.float32)
            scale = jnp.where(info[:, 2:3] == own_expert, info[:, 0:1] + info[:, 1:2], 0.0)
        c_g(r, i).wait_recv()
        for j in range(2):
            g, u = (
                gsend_ref[i, part, c:c + hw].astype(jnp.float32)
                + grecv_ref[i, part, c:c + hw].astype(jnp.float32)
                for c in (j * hw, hidden + j * hw)
            )
            if i == 0:
                g, u = g * scale, u * scale
            col = i * hidden + j * hw
            hid_ref[part, col:col + hw] = (g / (1.0 + jnp.exp(-g)) * u).astype(jnp.bfloat16)

    def product(first, rows, col, width):
        return jnp.dot(
            hid_ref[pl.ds(first, rows), :], dn_ref[:, col:col + width],
            preferred_element_type=jnp.float32,
        )

    def piece(r, i):
        units = slice(i * hidden, (i + 1) * hidden)
        return jnp.dot(
            hid_ref[pl.ds(*groups[r]), units], dn_ref[units, :],
            preferred_element_type=jnp.float32,
        )

    def block(b):
        return pl.ds(pl.multiple_of(b * tr, tr), tr)

    def c_xy(kind, d):
        src, dst, dev = ((sa1, ra1, xn), (sb1, rb1, yn), (sa2, ra2, yn), (sb2, rb2, xn))[kind % 4]
        rows = pl.ds(pl.multiple_of((line if kind >= 4 else 0) + d * tr, tr), tr)
        return pltpu.make_async_remote_copy(
            src_ref=src.at[rows], dst_ref=dst.at[rows],
            send_sem=send.at[1],
            recv_sem=early_recv.at[kind] if kind < 2 else xy_recv.at[kind - 2, d],
            device_id=dev, device_id_type=mesh_id,
        )

    order = (3 - 3 * (z // 2), 2 * (1 - z % 2) + z // 2, 1 + z % 2, z)

    def arrived(sem, part):
        pltpu.make_async_copy(part, part, sem).wait()

    def c_c(first, count, d):
        return pltpu.make_async_remote_copy(
            src_ref=cs.at[pl.ds(first, count), d], dst_ref=cr.at[z, pl.ds(first, count)],
            send_sem=send.at[3], recv_sem=c_recv.at[first],
            device_id=at(d * 4 + y * 2 + x), device_id_type=mesh_id,
        )

    def along(first, count, res):
        rows = slice(first * line, (first + count) * line)
        acc_ref[rows, both:] = res
        cs[first:first + count] = res.astype(jnp.bfloat16).reshape(count, zn, tr, half - both)
        for d in order[:zn - 1]:
            c_c(first, count, d).start()

    gate_up(0)
    activate(0, 0)
    activate(0, 1)
    for c in dloads:
        c.wait()
    along(0, 1, product(0, line, both, half - both))
    @pl.when(z - zn + 1 >= 0)
    def _():
        relay(jnp.maximum(z - zn + 1, 0))

    @pl.when(z + zn - 1 <= zn - 1)
    def _():
        relay(jnp.minimum(z + zn - 1, zn - 1))

    far_wait(0, 0)
    far_wait(1, 0)
    gate_up(1)
    activate(1, 0)
    acc_ref[line:3 * line, :] = piece(1, 0)
    activate(1, 1)
    res = acc_ref[line:3 * line, :] + piece(1, 1)
    sa1[0:line, :] = res[line:, :third].astype(jnp.bfloat16)
    sb1[0:line, :] = res[:line, third:both].astype(jnp.bfloat16)
    for k in range(zn):
        c_xy(0, order[k]).start()
        c_xy(1, order[k]).start()
    along(1, 2, res[:, both:])
    acc_ref[line:2 * line, 0:third] = res[:line, :third]
    acc_ref[2 * line:3 * line, third:both] = res[line:, third:both]
    far_wait(0, 1)
    far_wait(1, 1)
    gate_up(2)
    activate(2, 0)
    acc_ref[3 * line:, :] = piece(2, 0)
    activate(2, 1)
    res = acc_ref[3 * line:, :] + piece(2, 1)
    along(3, 1, res[:, both:])
    sa1[line:2 * line, :] = res[:, :third].astype(jnp.bfloat16)
    sb1[line:2 * line, :] = res[:, third:both].astype(jnp.bfloat16)
    for k in range(zn):
        c_xy(4, order[k]).start()
        c_xy(5, order[k]).start()
    acc_ref[0:line, 0:both] = product(0, line, 0, both)

    def shifted(base, d):
        return pl.ds(pl.multiple_of(base + d * tr, tr), tr)

    def second(d):
        c_xy(4, d).wait_recv()
        sa2[block(d), :] = (
            acc_ref[shifted(line, d), 0:third] + ra1[shifted(line, d), :].astype(jnp.float32)
        ).astype(jnp.bfloat16)
        c_xy(2, d).start()
        c_xy(5, d).wait_recv()
        sb2[block(d), :] = (
            acc_ref[shifted(2 * line, d), third:both] + rb1[shifted(line, d), :].astype(jnp.float32)
        ).astype(jnp.bfloat16)
        c_xy(3, d).start()

    def c_z(h, d):
        cols = pl.ds(h * third, third)
        return pltpu.make_async_remote_copy(
            src_ref=zsend.at[block(d), cols], dst_ref=zrecv.at[own, cols],
            send_sem=send.at[2], recv_sem=z_recv.at[h],
            device_id=at(d * 4 + y * 2 + x), device_id_type=mesh_id,
        )

    def summed(c):
        total = acc_ref[shifted(c * line, z), both:]
        for b in order[:zn - 1]:
            total = total + cr[b, c].astype(jnp.float32)
        return total

    def c_p(c):
        return pltpu.make_async_remote_copy(
            src_ref=ps.at[c - 1], dst_ref=pr.at[c - 1],
            send_sem=send.at[4], recv_sem=p_recv.at[0],
            device_id=(yn, xn, diag)[c - 1], device_id_type=mesh_id,
        )

    def settled(h, d):
        cols = slice(h * third, (h + 1) * third)
        first, r1, r2 = ((0, ra1, ra2), (1, rb1, rb2))[h]
        c_xy(first + 2, d).wait_recv()
        return acc_ref[block(d), cols] + r1[block(d), :].astype(jnp.float32) + r2[
            block(d), :
        ].astype(jnp.float32)

    for k in range(zn):
        second(order[k])
    for first, count in ((0, 1), (1, 2), (3, 1)):
        arrived(c_recv.at[first], cr.at[pl.ds(0, zn - 1), pl.ds(0, count)])
    for c in (1, 2, 3):
        ps[c - 1] = summed(c).astype(jnp.bfloat16)
        c_p(c).start()
    arrived(early_recv.at[0], ra1.at[pl.ds(0, line)])
    arrived(early_recv.at[1], rb1.at[pl.ds(0, line)])
    for k in range(zn - 1):
        d = order[k]
        for h in range(2):
            zsend[block(d), h * third:(h + 1) * third] = settled(h, d).astype(jnp.bfloat16)
            c_z(h, d).start()

    total = summed(0)
    arrived(p_recv.at[0], pr)
    for c in range(3):
        total = total + pr[c].astype(jnp.float32)
    out_ref[:, both:] = total.astype(out_ref.dtype)
    for h in range(2):
        cols = slice(h * third, (h + 1) * third)
        total = settled(h, z)
        arrived(z_recv.at[h], zrecv.at[pl.ds(0, line - tr), pl.ds(h * third, third)])
        for b in order[:zn - 1]:
            total = total + zrecv[block(b), cols].astype(jnp.float32)
        out_ref[:, cols] = total.astype(out_ref.dtype)

    def sent(sem, part):
        pltpu.make_async_remote_copy(
            src_ref=part, dst_ref=part, send_sem=sem, recv_sem=z_recv.at[0],
            device_id=partner, device_id_type=mesh_id,
        ).wait_send()

    for b in range(zn):
        @pl.when(jnp.logical_and(z < zn - 1, b == z))
        def _():
            sent(ag_send.at[1], x_ref.at[pl.ds(0, (b + 1) * tr)])

        @pl.when(jnp.logical_and(z > 0, b == z))
        def _():
            sent(ag_send.at[2], x_ref.at[pl.ds(0, (zn - b) * tr)])

    sent(ag_send.at[0], x_ref.at[pl.ds(0, 3 * line)])
    sent(send.at[0], gsend_ref)
    sent(send.at[1], x_ref.at[pl.ds(0, 3 * line), pl.ds(0, both)])
    sent(send.at[3], cs.at[pl.ds(0, zn - 1)])
    sent(send.at[4], ps)
    sent(send.at[2], zsend.at[pl.ds(0, line - tr)])


def fused_local(
    tokens, expert_ids, router_score, expert_gate_up, expert_down, shared_gate_up, shared_down
):
    tr, half = tokens.shape
    n = lax.axis_size("ep")
    zn = n // 4
    hidden = expert_down.shape[0]
    rows = n * tr
    line = zn * tr
    third = half * 6 // 20 // 128 * 128
    bf, f32 = jnp.bfloat16, jnp.float32
    vm = pl.BlockSpec(memory_space=pltpu.VMEM)
    hbm = pl.BlockSpec(memory_space=pltpu.HBM)
    dma = pltpu.SemaphoreType.DMA
    return pl.pallas_call(
        functools.partial(layer_kernel, zn),
        out_shape=pltpu.VMEM((tr, half), bf),
        in_specs=[hbm] * 7,
        out_specs=vm,
        scratch_shapes=[
            pltpu.VMEM((rows, half + META), bf),
            pltpu.VMEM((2, half, 2, hidden), bf),
            pltpu.VMEM((half, 4 * hidden), bf),
            pltpu.VMEM((2 * hidden, half), bf),
            pltpu.VMEM((2, rows, 2 * hidden), bf),
            pltpu.VMEM((2, rows, 2 * hidden), bf),
            pltpu.VMEM((rows, 2 * hidden), bf),
            pltpu.VMEM((2 * line, third), bf), pltpu.VMEM((2 * line, third), bf),
            pltpu.VMEM((2 * line, third), bf), pltpu.VMEM((2 * line, third), bf),
            pltpu.VMEM((line, third), bf), pltpu.VMEM((line, third), bf),
            pltpu.VMEM((line, third), bf), pltpu.VMEM((line, third), bf),
            pltpu.VMEM((rows, half), f32),
            pltpu.VMEM((line, 2 * third), bf), pltpu.VMEM((line, 2 * third), bf),
            pltpu.VMEM((4, zn, tr, half - 2 * third), bf), pltpu.VMEM((zn, 4, tr, half - 2 * third), bf),
            pltpu.VMEM((3, tr, half - 2 * third), bf), pltpu.VMEM((3, tr, half - 2 * third), bf),
            pltpu.VMEM((1, tr), jnp.int32), pltpu.VMEM((1, tr), f32), dma((3,)),
            dma((2, KCHUNKS)), dma((2,)), dma((3,)), dma((6, zn)), dma((2, 2)), dma((5,)), dma((3, 2)),
            dma((2,)), dma((4, zn)), dma((2,)), dma((4,)), dma((1,)),
        ],
        compiler_params=pltpu.CompilerParams(
            collective_id=0, has_side_effects=True, vmem_limit_bytes=56 * 2**20
        ),
    )(
        tokens, expert_ids.reshape(1, tr), router_score.reshape(1, tr),
        expert_gate_up, expert_down, shared_gate_up, shared_down,
    )


def slot_ranks(token_ids, experts):
    onehot = (token_ids[..., None] == jnp.arange(experts, dtype=jnp.int32)).astype(jnp.int32)
    before = jnp.cumsum(onehot, axis=-2) - onehot
    return jnp.sum(before * onehot, axis=-1)


def local_mlp(slot_rows, expert_gate_up, expert_down):
    hidden_width = expert_down.shape[0]
    gate_cols = expert_gate_up.reshape(expert_gate_up.shape[0], 2 * hidden_width)
    gate_up_sum = jnp.dot(slot_rows, gate_cols, preferred_element_type=jnp.float32)
    gate_up_sum = lax.psum(gate_up_sum.astype(jnp.bfloat16), "sub").astype(jnp.float32)
    gate_up_sum = gate_up_sum.reshape(slot_rows.shape[0], 2, hidden_width)
    hidden = (jax.nn.silu(gate_up_sum[:, 0]) * gate_up_sum[:, 1]).astype(jnp.bfloat16)
    return jnp.dot(hidden, expert_down, preferred_element_type=jnp.float32).astype(jnp.bfloat16)


def local(
    tokens, expert_ids, router_score, expert_gate_up, expert_down, shared_gate_up, shared_down
):
    rows_here, half_width = tokens.shape
    rows_ep = lax.axis_size("ep")
    experts = rows_ep // EXP_ROWS
    capacity = min(rows_here, max(2, 3 * rows_here // experts))
    shared_width = shared_down.shape[0]
    shared_in = shared_gate_up.reshape(half_width, 2 * shared_width)
    routed_extra = None
    all_tokens, all_ids, all_scores = (
        lax.all_gather(tokens, "ep", axis=0, tiled=True),
        lax.all_gather(expert_ids, "ep", axis=0, tiled=True),
        lax.all_gather(router_score.astype(jnp.bfloat16), "ep", axis=0, tiled=True).astype(
            router_score.dtype
        ),
    )
    shared_sum = jnp.dot(all_tokens, shared_in, preferred_element_type=jnp.float32)
    token_ids = all_ids[:, 0].reshape(rows_ep, rows_here)
    position = slot_ranks(token_ids, experts)
    own_expert = lax.axis_index("ep") // EXP_ROWS
    row_index = lax.broadcasted_iota(jnp.int32, (rows_ep, rows_here), 0)
    slot_index = jnp.where(token_ids == own_expert, row_index * capacity + position, -1).reshape(-1)
    slot_iota = lax.broadcasted_iota(jnp.int32, (rows_ep * capacity, rows_ep * rows_here), 0)
    select = (slot_iota == slot_index[None, :]).astype(jnp.bfloat16)
    weighted = (jax.nn.sigmoid(all_scores) * all_tokens.astype(jnp.float32)).astype(jnp.bfloat16)
    slot_rows = jnp.dot(select, weighted, preferred_element_type=jnp.float32).astype(jnp.bfloat16)
    results = local_mlp(slot_rows, expert_gate_up, expert_down)
    routed_extra = lax.dot_general(
        select, results, (((0,), (0,)), ((), ())), preferred_element_type=jnp.float32
    )
    shared_sum = lax.psum(shared_sum.astype(jnp.bfloat16), "sub").astype(jnp.float32)
    shared_sum = shared_sum.reshape(-1, 2, shared_width)
    shared_hidden = (jax.nn.silu(shared_sum[:, 0]) * shared_sum[:, 1]).astype(jnp.bfloat16)
    partial_value = jnp.dot(shared_hidden, shared_down, preferred_element_type=jnp.float32)
    partial_value = partial_value + routed_extra
    mixed = lax.psum_scatter(partial_value, "ep", scatter_dimension=0, tiled=True)
    return mixed.astype(jnp.bfloat16)


def solution(mesh):
    placed = (
        P(("rep", "ep"), "sub"),
        P(("rep", "ep"), None),
        P(("rep", "ep"), None),
        P("sub", None, "ep"),
        P("ep", "sub"),
        P("sub", None, "ep"),
        P("ep", "sub"),
    )
    fused = mesh.shape["ep"] == GRID_ROWS
    return jax.shard_map(
        fused_local if fused else local, mesh=mesh, in_specs=placed, out_specs=P(("rep", "ep"), "sub"), check_vma=False
    )
```
